32 devices in a mesh: group: 4 (over y, core), local: 8 (over z, x).
Axes of the slice: x: 2, y: 2, z: 4, core: 2. Of those that a mesh axis runs over, the one named last changes fastest.
Arguments:
- lookup_grads: bfloat16 [262144, 256], P(('group', 'local')), may hold values from -0.29882812 to 0.29882812
- slot_index: int32 [2, 262144], P(None, ('group', 'local')), may hold values from 0 to 511, as said below
- unique_rows: int32 [2, 2048], P(None, ('group', 'local')), may hold values from -1 to 32767, as said below
- tables: float32 [2, 32768, 256], P(None, ('group', 'local')), may hold values from -6 to 6
- accums: float32 [2, 32768], P(None, ('group', 'local')), may hold values from 0.01 to 1
Outputs:
- new_tables: float32 [2, 32768, 256], P(None, ('group', 'local'))
- new_accums: float32 [2, 32768], P(None, ('group', 'local'))
The draws below stay inside these ranges and needn't reach their ends.
Inputs may be any that keep to these rules, and one draw needn't show every extreme that they name: slot_index[t, i] names a slot of lookup i's group list whose entry in unique_rows[t] is not -1. `unique_rows`: table row p is owned by device p // 1024, which is device (group p // 8192, local p // 1024 % 8). Group g's list is entries g * 512 to (g + 1) * 512 - 1; its block l of 64 entries consists of 4 buckets of 16 entries, bucket h holding only rows owned by device (group h, local l), the used entries first and -1 after them. Rows within a group's list are distinct. In every draw and table some device (group h, local l) gets a full bucket from every group.
All inputs are finite; a program needn't handle non-finite values.
Results may differ from the reference program's by a relative error of at most 0.0003.
Values sent between devices are 32-bit elements; how exact they have to be, the bound alone decides.
A program may use at most 64 MiB of HBM per device.

```python
import math
import jax
import jax.numpy as jnp
from jax import lax

EMB = 256
LOOK_DEV = 8192
CAP = 16
ROWS_DEV = 1024
SLOTS = 64
GROUP_SLOTS = 512
ALL_SLOTS = 2048
LOOKUPS = 262144
ROWS = 32768
N_GROUP = 4
N_LOCAL = 8


def shared_layout(key):
    base_key = jax.random.fold_in(key, 7)
    count_key, pick_key, offset_key, stride_key = jax.random.split(base_key, 4)
    bucket_shape = (2, N_GROUP, N_LOCAL, N_GROUP)
    live_count = jax.random.randint(count_key, bucket_shape, (CAP + 3) // 4, CAP + 1)
    local_pick = jax.random.randint(jax.random.fold_in(pick_key, 1), (2,), 0, N_LOCAL)
    group_pick = jax.random.randint(jax.random.fold_in(pick_key, 2), (2,), 0, N_GROUP)
    local_iota = jnp.arange(N_LOCAL)[None, None, :, None]
    group_iota = jnp.arange(N_GROUP)[None, None, None, :]
    marked = (local_iota == local_pick[:, None, None, None]) & (group_iota == group_pick[:, None, None, None])
    live_count = jnp.where(marked, CAP, live_count)
    return (live_count, offset_key, stride_key)


def draw_unique_rows(key, part):
    live_count, offset_key, stride_key = shared_layout(key)
    bucket_shape = (2, N_GROUP, N_LOCAL, N_GROUP)
    offset = jax.random.randint(offset_key, bucket_shape, 0, ROWS_DEV)
    stride = 2 * jax.random.randint(stride_key, bucket_shape, 0, max(ROWS_DEV // 2, 1)) + 1
    position = jnp.arange(CAP)
    local_rows = (offset[..., None] + stride[..., None] * position) % ROWS_DEV
    owners = jnp.arange(N_GROUP)[None, None, None, :] * N_LOCAL + jnp.arange(N_LOCAL)[None, None, :, None]
    row_ids = owners[..., None] * ROWS_DEV + local_rows
    row_ids = jnp.where(position < live_count[..., None], row_ids, -1)
    return row_ids.reshape(2, ALL_SLOTS).astype(jnp.int32)


def draw_slot_index(key, part):
    live_count, offset_key, stride_key = shared_layout(key)
    slot_key = jax.random.fold_in(key, 19)
    first_key, second_key, third_key = jax.random.split(slot_key, 3)
    local_choice = jax.random.randint(first_key, (2, LOOKUPS), 0, N_LOCAL)
    group_choice = jax.random.randint(second_key, (2, LOOKUPS), 0, N_GROUP)
    random_bits = jax.random.randint(third_key, (2, LOOKUPS), 0, 2 ** 20)
    group_of = jnp.arange(LOOKUPS) // (LOOK_DEV * N_LOCAL)
    table_of = jnp.arange(2)[:, None]
    available = live_count[table_of, group_of[None, :], local_choice, group_choice]
    slots = local_choice * SLOTS + group_choice * CAP + random_bits % available
    return slots.astype(jnp.int32)


def block_scale(key, shape, pieces, least, largest):
    factor_of, own = 1.0, jax.random.fold_in(key, 6)
    for axis_at, blocks in pieces:
        steps = jnp.exp(jax.random.uniform(jax.random.fold_in(own, axis_at), (blocks,), jnp.float32, least / len(pieces), largest / len(pieces)))
        factor_of = factor_of * jnp.repeat(steps, shape[axis_at] // blocks).reshape([-1 if axis == axis_at else 1 for axis in range(len(shape))])
    return factor_of


def noise(stream_key, extent, spread, bound, cuts=(), kind=jnp.bfloat16):
    result = spread * jax.random.normal(stream_key, extent, jnp.float32)
    if cuts:
        result = result * block_scale(stream_key, extent, cuts, -0.22, 0.18)
    return jnp.clip(result, -bound, bound).astype(kind)


def setup_inputs(seed: int = 0) -> dict:
    arg_keys = jax.random.split(jax.random.key(seed), 6)
    return {
        "lookup_grads": noise(arg_keys[0], (LOOKUPS, EMB), 0.05, 0.29882812, ((0, 32),)),
        "slot_index": draw_slot_index(jax.random.fold_in(arg_keys[5], 71), 0),
        "unique_rows": draw_unique_rows(jax.random.fold_in(arg_keys[5], 71), 0),
        "tables": noise(arg_keys[3], (2, ROWS, EMB), 1.0, 6.0, ((1, 32),), jnp.float32),
        "accums": jnp.clip(jnp.exp(math.log(1.0) - 4.6051702 * jax.random.uniform(arg_keys[4], (2, ROWS), jnp.float32) ** block_scale(arg_keys[4], (2, ROWS), ((1, 32),), -0.2, 0.2)), 0.01, 1.0),
    }


learning_rate = 0.1
epsilon = 1e-08

def reference(lookup_grads, slot_index, unique_rows, tables, accums):
    per_group = LOOK_DEV * N_LOCAL
    grouped = lookup_grads.reshape(N_GROUP, per_group, EMB)
    slots_grouped = jnp.transpose(slot_index.reshape(2, N_GROUP, per_group), (1, 0, 2))

    def group_total(inputs):
        gradients, slots_here = inputs
        wide = gradients.astype(jnp.float32)
        first = jax.ops.segment_sum(wide, slots_here[0], num_segments=GROUP_SLOTS)
        second = jax.ops.segment_sum(wide, slots_here[1], num_segments=GROUP_SLOTS)
        return jnp.stack([first, second])
    group_sums = lax.map(group_total, (grouped, slots_grouped))
    group_sums = jnp.transpose(group_sums, (1, 0, 2, 3)).reshape(2, ALL_SLOTS, EMB)
    new_tables = []
    new_accums = []
    for table_index in range(2):
        row_numbers = unique_rows[table_index]
        targets = jnp.where(row_numbers < 0, ROWS, row_numbers).astype(jnp.int32)
        row_grads = jnp.zeros((ROWS, EMB), jnp.float32).at[targets].add(group_sums[table_index], mode='drop')
        accum_new = accums[table_index] + lax.optimization_barrier(jnp.mean(row_grads * row_grads, axis=1))
        table_new = tables[table_index] - learning_rate * row_grads / (jnp.sqrt(accum_new)[:, None] + epsilon)
        new_tables.append(table_new)
        new_accums.append(accum_new)
    return (jnp.stack(new_tables), jnp.stack(new_accums))
```

```python
import functools

import jax
import jax.numpy as jnp
from jax import lax
from jax.experimental import pallas as pl
from jax.experimental.pallas import tpu as pltpu
from jax.sharding import PartitionSpec as P

learning_rate = 0.1
epsilon = 1e-08
MESH = pl.DeviceIdType.MESH
PIECES = 2
BLOCKS = 4


def split_bf16(x):
    high = x.astype(jnp.bfloat16)
    rest = x - high.astype(jnp.float32)
    middle = rest.astype(jnp.bfloat16)
    low = (rest - middle.astype(jnp.float32)).astype(jnp.bfloat16)
    return jnp.concatenate([high, middle, low], axis=0)


def exchange_kernel(
    n_group, n_local, chunk, grads_hbm, index_hbm, rows_hbm, tables_hbm, accums_hbm,
    parts_ref, onehot_ref, tables_ref, new_accums_ref,
    grads, index, rows, accums, sums, pair, relay, recv, rows_recv, acc, same_ref, hit_ref, old_ref,
    grad_sems, index_sem, rows_sem, tables_sem, accums_sem, pair_sems, relay_sems,
    pair_send_sem, send_sem, recv_sem, row_send_sem, row_recv_sem, near_sem, far_sem,
):
    group, local = lax.axis_index("group"), lax.axis_index("local")
    look, width = grads.shape
    capacity = sums.shape[2]
    slots = rows.shape[1]
    rows_dev = tables_hbm.shape[1]
    n_chunk = look // chunk
    peers = n_local // BLOCKS
    buckets = peers * n_group
    rows_block = buckets * capacity
    places = 2 + peers
    block_me, peer_me = local // peers, lax.rem(local, peers)
    half = block_me // 2
    inner = lax.rem(block_me + half, 2)
    near = block_me + 1 - 2 * lax.rem(block_me, 2)
    across = BLOCKS - 1 - block_me
    order = (BLOCKS - 1 - 3 * half, 2 - half, near, block_me)

    def signal_near(sem):
        for o in range(1, peers):
            pl.semaphore_signal(
                sem, inc=1, device_id={"group": group, "local": block_me * peers + lax.rem(peer_me + o, peers)},
                device_id_type=MESH,
            )
        pl.semaphore_signal(
            sem, inc=1, device_id={"group": group, "local": near * peers + peer_me}, device_id_type=MESH
        )

        @pl.when(inner == 1)
        def _():
            pl.semaphore_signal(
                sem, inc=1, device_id={"group": group, "local": across * peers + peer_me}, device_id_type=MESH
            )

        for o in range(1, n_group):
            pl.semaphore_signal(
                sem, inc=1, device_id={"group": lax.rem(group + o, n_group), "local": local}, device_id_type=MESH
            )

    met = peers - 1 + 1 + n_group - 1 + inner

    index_load = pltpu.make_async_copy(index_hbm, index, index_sem)
    rows_load = pltpu.make_async_copy(rows_hbm, rows, rows_sem)
    tables_load = pltpu.make_async_copy(tables_hbm, tables_ref, tables_sem)
    accums_load = pltpu.make_async_copy(accums_hbm, accums, accums_sem)

    def load(k):
        at = pl.ds(k * chunk, chunk)
        return pltpu.make_async_copy(grads_hbm.at[at], grads.at[at], grad_sems.at[k])

    index_load.start()
    for k in range(n_chunk):
        load(k).start()
    rows_load.start()
    accums_load.start()
    barrier = pltpu.get_barrier_semaphore()
    signal_near(barrier)

    def send_pair(step, o, h):
        to = order[step] * peers + lax.rem(peer_me + o, peers)
        return pltpu.make_async_remote_copy(
            src_ref=sums.at[to * n_group + h],
            dst_ref=pair.at[(step * n_group + h) * (peers - 1) + (peers - 1 - o)],
            send_sem=pair_send_sem, recv_sem=pair_sems.at[step * n_group + h],
            device_id={"group": group, "local": block_me * peers + lax.rem(peer_me + o, peers)},
            device_id_type=MESH,
        )

    def send_relay(step, h):
        return pltpu.make_async_remote_copy(
            src_ref=sums.at[(order[step] * peers + peer_me) * n_group + h], dst_ref=relay.at[step * n_group + h],
            send_sem=send_sem, recv_sem=relay_sems.at[step * n_group + h],
            device_id={"group": group, "local": near * peers + peer_me}, device_id_type=MESH,
        )

    def send_bucket(l, h, place):
        return pltpu.make_async_remote_copy(
            src_ref=sums.at[l * n_group + h], dst_ref=recv.at[group * places + place],
            send_sem=send_sem, recv_sem=recv_sem,
            device_id={"group": h, "local": l}, device_id_type=MESH,
        )

    def send_rows(h):
        return pltpu.make_async_remote_copy(
            src_ref=rows, dst_ref=rows_recv.at[group],
            send_sem=row_send_sem, recv_sem=row_recv_sem,
            device_id={"group": h, "local": local}, device_id_type=MESH,
        )

    def sum_part(step, start, stop):
        block = order[step]
        targets = lax.broadcasted_iota(jnp.int32, (rows_block, chunk), 0) + block * rows_block

        def body(k, c):
            if step == 0:
                load(k).wait()
            at = pl.ds(pl.multiple_of(k * chunk, chunk), chunk)
            onehot = jnp.concatenate(
                [jnp.where(index[t : t + 1, at] == targets, 1.0, 0.0).astype(jnp.bfloat16) for t in range(2)],
                axis=0,
            )
            acc[...] += jnp.dot(onehot, grads[at, :], preferred_element_type=jnp.float32)
            return c

        if start == 0:
            acc[...] = jnp.zeros_like(acc)
        lax.fori_loop(start, stop, body, 0)
        if stop == n_chunk:
            for t in range(2):
                sums[pl.ds(block * buckets, buckets), t] = acc[t * rows_block : (t + 1) * rows_block, :].reshape(
                    buckets, capacity, width
                )

    def start_pairs(step):
        def one(i, c):
            send_pair(step, 1 + i // n_group, lax.rem(group + lax.rem(i, n_group), n_group)).start()
            return c

        lax.fori_loop(0, (peers - 1) * n_group, one, 0)

    def add_pairs(step, h):
        first = (step * n_group + h) * (peers - 1)
        pltpu.make_async_remote_copy(
            src_ref=pair.at[pl.ds(first, peers - 1)], dst_ref=pair.at[pl.ds(first, peers - 1)],
            send_sem=pair_send_sem, recv_sem=pair_sems.at[step * n_group + h],
            device_id={"group": group, "local": local}, device_id_type=MESH,
        ).wait_recv()
        at = (order[step] * peers + peer_me) * n_group + h
        total = sums[at]
        for p in range(peers - 1):
            total = total + pair[first + p]
        sums[at] = total

    def pass_relay(step):
        def one(i, c):
            h = lax.rem(group + i, n_group)
            add_pairs(step, h)

            @pl.when(inner == 0)
            def _():
                send_relay(step, h).start()

            return c

        lax.fori_loop(0, n_group, one, 0)

    def finish_relay(step, h):
        @pl.when(inner == 1)
        def _():
            pltpu.make_async_remote_copy(
                src_ref=relay.at[step * n_group + h], dst_ref=relay.at[step * n_group + h],
                send_sem=send_sem, recv_sem=relay_sems.at[step * n_group + h],
                device_id={"group": group, "local": local}, device_id_type=MESH,
            ).wait_recv()
            to = order[step] * peers + peer_me
            sums[to * n_group + h] = sums[to * n_group + h] + relay[step * n_group + h]
            send_bucket(to, h, 0).start()

    index_load.wait()
    sum_part(0, 0, n_chunk)
    pl.semaphore_wait(barrier, met)
    start_pairs(0)
    signal_near(near_sem)
    tables_load.start()
    rows_load.wait()

    def row_step(o, c):
        send_rows(lax.rem(group + o, n_group)).start()
        return c

    lax.fori_loop(1, n_group, row_step, 0)
    sum_part(1, 0, n_chunk)
    start_pairs(1)
    pl.semaphore_wait(near_sem, met)

    @pl.when(inner == 1)
    def _():
        pl.semaphore_signal(
            far_sem, inc=1, device_id={"group": group, "local": across * peers + peer_me}, device_id_type=MESH
        )

    sum_part(2, 0, n_chunk)
    start_pairs(2)
    pass_relay(0)
    middle = n_chunk // 2
    if middle:
        sum_part(3, 0, middle)

    @pl.when(inner == 1)
    def _():
        pl.semaphore_wait(far_sem, 1)

    def finish_first(i, c):
        finish_relay(0, lax.rem(group + i, n_group))
        return c

    lax.fori_loop(0, n_group, finish_first, 0)
    pass_relay(1)
    sum_part(3, middle, n_chunk)

    def own_step(i, c):
        l = block_me * peers + lax.rem(peer_me + 1 + i // n_group, peers)
        send_bucket(l, lax.rem(group + 1 + i, n_group), 2 + peer_me).start()
        return c

    lax.fori_loop(0, buckets - 1, own_step, 0)
    recv[group * places + 2 + peer_me] = sums[local * n_group + group]

    def last_step(i, c):
        h = lax.rem(group + i, n_group)
        add_pairs(2, h)
        send_bucket(order[2] * peers + peer_me, h, 1).start()
        finish_relay(1, h)
        return c

    lax.fori_loop(0, n_group, last_step, 0)

    row_wait = pltpu.make_async_remote_copy(
        src_ref=rows_recv.at[pl.ds(0, n_group - 1)], dst_ref=rows_recv.at[pl.ds(0, n_group - 1)],
        send_sem=row_send_sem, recv_sem=row_recv_sem,
        device_id={"group": group, "local": local}, device_id_type=MESH,
    )
    rows_recv[group] = rows[...]
    row_wait.wait_recv()
    accums_load.wait()
    base = ((group * n_local + local) * rows_dev).astype(jnp.float32)
    slot_at = lax.broadcasted_iota(jnp.int32, (capacity, slots), 0)
    lane_at = lax.broadcasted_iota(jnp.int32, (capacity, slots), 1)
    first_at = lax.broadcasted_iota(jnp.int32, (slots, slots), 0)
    second_at = lax.broadcasted_iota(jnp.int32, (slots, slots), 1)
    row_lane = lax.broadcasted_iota(jnp.int32, (slots, rows_dev), 1).astype(jnp.float32)
    for t in range(2):
        columns = []
        for g in range(n_group):
            mine = lane_at == slot_at + group * capacity
            numbers = rows_recv[g, t : t + 1, :].astype(jnp.float32)
            columns.append(jnp.sum(jnp.where(mine, numbers, 0.0), axis=1, keepdims=True))
        column = jnp.concatenate(columns, axis=0)
        column = jnp.where(column < 0.0, -1.0, column - base)
        as_row = jnp.sum(jnp.where(first_at == second_at, column, 0.0), axis=0, keepdims=True)
        same = jnp.where(column == as_row, 1.0, 0.0)
        same_ref[t] = jnp.concatenate([same] * 3, axis=1).astype(jnp.bfloat16)
        hit = jnp.where(row_lane == column, 1.0, 0.0)
        hit_ref[t] = hit
        old_ref[t] = jnp.broadcast_to(jnp.sum(hit * accums[t : t + 1, :], axis=1, keepdims=True), old_ref.shape[1:])
        earlier = jnp.max(jnp.where(first_at < second_at, same, 0.0), axis=0, keepdims=True)
        target = jnp.where(earlier > 0.0, -1.0, as_row)
        target = jnp.concatenate([target] * 3, axis=1)
        piece = rows_dev // 8
        for i in range(8):
            piece_row = lax.broadcasted_iota(jnp.int32, (piece, 3 * slots), 0).astype(jnp.float32) + float(i * piece)
            onehot_ref[t, i * piece : (i + 1) * piece] = jnp.where(piece_row == target, 1.0, 0.0).astype(jnp.bfloat16)

    row_wait.wait_send()
    tables_load.wait()
    pair_parts = (BLOCKS - 1) * n_group * (peers - 1)
    pltpu.make_async_remote_copy(
        src_ref=pair.at[pl.ds(0, pair_parts)], dst_ref=pair.at[pl.ds(0, pair_parts)],
        send_sem=pair_send_sem, recv_sem=recv_sem,
        device_id={"group": group, "local": local}, device_id_type=MESH,
    ).wait_send()
    sent = (BLOCKS - 1) * n_group + buckets - 1
    pltpu.make_async_remote_copy(
        src_ref=sums.at[pl.ds(0, sent)], dst_ref=sums.at[pl.ds(0, sent)],
        send_sem=send_sem, recv_sem=recv_sem,
        device_id={"group": group, "local": local}, device_id_type=MESH,
    ).wait_send()
    parts = n_group * places - 1
    pltpu.make_async_remote_copy(
        src_ref=recv.at[pl.ds(0, parts)], dst_ref=recv.at[pl.ds(0, parts)],
        send_sem=send_sem, recv_sem=recv_sem,
        device_id={"group": group, "local": local}, device_id_type=MESH,
    ).wait_recv()
    for t in range(2):
        lists = []
        for g in range(n_group):
            total = recv[g * places, t]
            for p in range(1, places):
                total = total + recv[g * places + p, t]
            lists.append(total)
        totals = jnp.dot(
            same_ref[t], split_bf16(jnp.concatenate(lists, axis=0)), preferred_element_type=jnp.float32
        )
        squares = jnp.mean(totals * totals, axis=1, keepdims=True)
        added = jnp.max(hit_ref[t] * squares, axis=0, keepdims=True)
        new_accums_ref[t : t + 1, :] = accums[t : t + 1, :] + added
        change = learning_rate * totals / (jnp.sqrt(old_ref[t][:, 0:1] + squares) + epsilon)
        parts_ref[t] = split_bf16(change)


def update_kernel(parts_ref, onehot_ref, tables_ref, accums_ref, new_tables_hbm, new_accums_hbm, new, out_sems, accums_sem):
    rows_dev = tables_ref.shape[1]
    piece = rows_dev // PIECES
    accums_out = pltpu.make_async_copy(accums_ref, new_accums_hbm, accums_sem)
    accums_out.start()

    def out(t, i):
        at = pl.ds(i * piece, piece)
        return pltpu.make_async_copy(new.at[t, at], new_tables_hbm.at[t, at], out_sems.at[t, i])

    for t in range(2):
        for i in range(PIECES):
            at = slice(i * piece, (i + 1) * piece)
            new[t, at] = tables_ref[t, at] - jnp.dot(
                onehot_ref[t, at], parts_ref[t], preferred_element_type=jnp.float32
            )
            out(t, i).start()
    accums_out.wait()
    for t in range(2):
        for i in range(PIECES):
            out(t, i).wait()


def local_step(n_group, n_local, lookup_grads, slot_index, unique_rows, tables, accums):
    look, width = lookup_grads.shape
    slots = unique_rows.shape[1]
    capacity = slots // n_group
    n_dev = n_group * n_local
    rows_dev = tables.shape[1]
    chunk = min(4096, look)
    peers = n_local // BLOCKS
    block_rows = 2 * (slots * n_local // BLOCKS)
    vmem = pl.BlockSpec(memory_space=pltpu.VMEM)
    hbm = pl.BlockSpec(memory_space=pltpu.HBM)
    dma = pltpu.SemaphoreType.DMA
    regular = pltpu.SemaphoreType.REGULAR
    prepared = pl.pallas_call(
        functools.partial(exchange_kernel, n_group, n_local, chunk),
        out_shape=(
            pltpu.VMEM((2, 3 * slots, width), jnp.bfloat16),
            pltpu.VMEM((2, rows_dev, 3 * slots), jnp.bfloat16),
            pltpu.VMEM(tables.shape, jnp.float32),
            pltpu.VMEM(accums.shape, jnp.float32),
        ),
        in_specs=[hbm] * 5,
        out_specs=(vmem, vmem, vmem, vmem),
        scratch_shapes=[
            pltpu.VMEM((look, width), jnp.bfloat16),
            pltpu.VMEM((2, look), jnp.int32),
            pltpu.VMEM((2, slots), jnp.int32),
            pltpu.VMEM((2, rows_dev), jnp.float32),
            pltpu.VMEM((n_dev, 2, capacity, width), jnp.float32),
            pltpu.VMEM(((BLOCKS - 1) * n_group * (peers - 1), 2, capacity, width), jnp.float32),
            pltpu.VMEM((2 * n_group, 2, capacity, width), jnp.float32),
            pltpu.VMEM((n_group * (2 + peers), 2, capacity, width), jnp.float32),
            pltpu.VMEM((n_group, 2, slots), jnp.int32),
            pltpu.VMEM((block_rows, width), jnp.float32),
            pltpu.VMEM((2, slots, 3 * slots), jnp.bfloat16),
            pltpu.VMEM((2, slots, rows_dev), jnp.float32),
            pltpu.VMEM((2, slots, 128), jnp.float32),
            dma((look // chunk,)), dma, dma, dma, dma,
            dma(((BLOCKS - 1) * n_group,)), dma((2 * n_group,)),
            dma, dma, dma, dma, dma, regular, regular,
        ],
        compiler_params=pltpu.CompilerParams(
            collective_id=0, has_side_effects=True, vmem_limit_bytes=48 * 2**20
        ),
        cost_estimate=pl.CostEstimate(flops=2 * 2 * look * width * slots * n_local, bytes_accessed=2 * look * width, transcendentals=0),
    )(*[pltpu.with_memory_space_constraint(x, pltpu.HBM) for x in (lookup_grads, slot_index, unique_rows, tables, accums)])
    return pl.pallas_call(
        update_kernel,
        out_shape=(
            jax.ShapeDtypeStruct(tables.shape, jnp.float32),
            jax.ShapeDtypeStruct(accums.shape, jnp.float32),
        ),
        in_specs=[vmem] * 4,
        out_specs=(hbm, hbm),
        scratch_shapes=[
            pltpu.VMEM((2, rows_dev, width), jnp.float32),
            dma((2, PIECES)), dma,
        ],
        compiler_params=pltpu.CompilerParams(vmem_limit_bytes=16 * 2**20),
    )(*prepared)


def solution(mesh):
    n_group, n_local = mesh.shape["group"], mesh.shape["local"]
    return jax.shard_map(
        functools.partial(local_step, n_group, n_local),
        mesh=mesh,
        in_specs=(
            P(("group", "local"), None),
            P(None, ("group", "local")),
            P(None, ("group", "local")),
            P(None, ("group", "local"), None),
            P(None, ("group", "local")),
        ),
        out_specs=(P(None, ("group", "local"), None), P(None, ("group", "local"))),
        check_vma=False,
    )
```

```python
import functools

import jax
import jax.numpy as jnp
from jax import lax
from jax.experimental import pallas as pl
from jax.experimental.pallas import tpu as pltpu
from jax.sharding import PartitionSpec as P

learning_rate = 0.1
epsilon = 1e-08
MESH = pl.DeviceIdType.MESH
PIECES = 2
BLOCKS = 4


def split_bf16(x):
    high = x.astype(jnp.bfloat16)
    rest = x - high.astype(jnp.float32)
    middle = rest.astype(jnp.bfloat16)
    low = (rest - middle.astype(jnp.float32)).astype(jnp.bfloat16)
    return jnp.concatenate([high, middle, low], axis=0)


def exchange_kernel(
    n_group, n_local, grads_hbm, index_hbm, rows_hbm, tables_hbm, accums_hbm,
    parts_ref, onehot_ref, tables_ref, new_accums_ref,
    grads, index, rows, accums, sums, pair, relay, recv, rows_recv, same_ref, hit_ref, old_ref,
    grads_sem, index_sem, rows_sem, tables_sem, accums_sem, pair_sems, relay_sems,
    pair_send_sem, send_sem, recv_sem, row_send_sem, row_recv_sem, near_sem, far_sem,
):
    group, local = lax.axis_index("group"), lax.axis_index("local")
    width = grads.shape[1]
    capacity = sums.shape[2]
    slots = rows.shape[1]
    rows_dev = tables_hbm.shape[1]
    peers = n_local // BLOCKS
    buckets = peers * n_group
    early = n_group // 2
    places = 3 + peers
    block_me, peer_me = local // peers, lax.rem(local, peers)
    half = block_me // 2
    inner = lax.rem(block_me + half, 2)
    near = block_me + 1 - 2 * lax.rem(block_me, 2)
    across = BLOCKS - 1 - block_me
    far_inner, far_outer = 2 - half, BLOCKS - 1 - 3 * half
    order = (
        far_outer + inner * (far_inner - far_outer), far_inner + inner * (far_outer - far_inner), near, block_me
    )

    def signal_near(sem):
        for o in range(1, peers):
            pl.semaphore_signal(
                sem, inc=1, device_id={"group": group, "local": block_me * peers + lax.rem(peer_me + o, peers)},
                device_id_type=MESH,
            )
        pl.semaphore_signal(
            sem, inc=1, device_id={"group": group, "local": near * peers + peer_me}, device_id_type=MESH
        )

        @pl.when(inner == 1)
        def _():
            pl.semaphore_signal(
                sem, inc=1, device_id={"group": group, "local": across * peers + peer_me}, device_id_type=MESH
            )

        for o in range(1, n_group):
            pl.semaphore_signal(
                sem, inc=1, device_id={"group": lax.rem(group + o, n_group), "local": local}, device_id_type=MESH
            )

    met = peers - 1 + 1 + n_group - 1 + inner

    index_load = pltpu.make_async_copy(index_hbm, index, index_sem)
    rows_load = pltpu.make_async_copy(rows_hbm, rows, rows_sem)
    tables_load = pltpu.make_async_copy(tables_hbm, tables_ref, tables_sem)
    accums_load = pltpu.make_async_copy(accums_hbm, accums, accums_sem)

    grads_load = pltpu.make_async_copy(grads_hbm, grads, grads_sem)

    index_load.start()
    grads_load.start()
    rows_load.start()
    accums_load.start()
    barrier = pltpu.get_barrier_semaphore()
    signal_near(barrier)

    def send_pair(step, o, h):
        to = order[step] * peers + lax.rem(peer_me + o, peers)
        return pltpu.make_async_remote_copy(
            src_ref=sums.at[to * n_group + h],
            dst_ref=pair.at[(step * n_group + h) * (peers - 1) + (peers - 1 - o)],
            send_sem=pair_send_sem, recv_sem=pair_sems.at[step * n_group + h],
            device_id={"group": group, "local": block_me * peers + lax.rem(peer_me + o, peers)},
            device_id_type=MESH,
        )

    def send_relay(h):
        return pltpu.make_async_remote_copy(
            src_ref=sums.at[(order[0] * peers + peer_me) * n_group + h], dst_ref=relay.at[h],
            send_sem=send_sem, recv_sem=relay_sems.at[h],
            device_id={"group": group, "local": near * peers + peer_me}, device_id_type=MESH,
        )

    def send_bucket(l, h, place):
        return pltpu.make_async_remote_copy(
            src_ref=sums.at[l * n_group + h], dst_ref=recv.at[group * places + place],
            send_sem=send_sem, recv_sem=recv_sem,
            device_id={"group": h, "local": l}, device_id_type=MESH,
        )

    def send_rows(h):
        return pltpu.make_async_remote_copy(
            src_ref=rows, dst_ref=rows_recv.at[group],
            send_sem=row_send_sem, recv_sem=row_recv_sem,
            device_id={"group": h, "local": local}, device_id_type=MESH,
        )

    def whole(block, o):
        at = (block * peers + lax.rem(peer_me + o, peers)) * n_group
        return at, at + early

    runs, events = [], {}

    def sum_runs(q):
        first, second = (
            functools.reduce(lambda x, k: jnp.where(q == k, runs[k][i], x), range(1, len(runs)), runs[0][i])
            for i in range(2)
        )
        row = lax.broadcasted_iota(jnp.int32, (early * capacity, 1), 0)
        targets = jnp.concatenate([row + first * capacity, row + second * capacity], axis=0)
        onehot = jnp.concatenate(
            [jnp.where(index[t : t + 1, :] == targets, 1.0, 0.0).astype(jnp.bfloat16) for t in range(2)], axis=0
        )
        total = jnp.dot(onehot, grads[...], preferred_element_type=jnp.float32)
        n_rows = early * capacity
        for t in range(2):
            for i, at in enumerate((first, second)):
                start = (2 * t + i) * n_rows
                sums[pl.ds(at, early), t] = total[start : start + n_rows, :].reshape(early, capacity, width)

    def turn(step, i):
        return jnp.where(order[step] == 0, i, lax.rem(i + 1, 2) * early + i // 2)

    def start_pairs(step):
        def one(i, c):
            send_pair(step, 1 + i // n_group, turn(step, lax.rem(i, n_group))).start()
            return c

        lax.fori_loop(0, (peers - 1) * n_group, one, 0)

    def add_pairs(step, h):
        first = (step * n_group + h) * (peers - 1)
        pltpu.make_async_remote_copy(
            src_ref=pair.at[pl.ds(first, peers - 1)], dst_ref=pair.at[pl.ds(first, peers - 1)],
            send_sem=pair_send_sem, recv_sem=pair_sems.at[step * n_group + h],
            device_id={"group": group, "local": local}, device_id_type=MESH,
        ).wait_recv()
        at = (order[step] * peers + peer_me) * n_group + h
        total = sums[at]
        for p in range(peers - 1):
            total = total + pair[first + p]
        sums[at] = total

    def pass_on(step, h, place):
        send_bucket(order[step] * peers + peer_me, h, place).start()

    def pass_first(h):
        add_pairs(0, h)
        pl.when(inner == 0)(lambda: send_relay(h).start())
        pl.when(inner == 1)(lambda: pass_on(0, h, 0))

    def pass_second(h):
        add_pairs(1, h)

        @pl.when(inner == 1)
        def _():
            pltpu.make_async_remote_copy(
                src_ref=relay.at[h], dst_ref=relay.at[h], send_sem=send_sem, recv_sem=relay_sems.at[h],
                device_id={"group": group, "local": local}, device_id_type=MESH,
            ).wait_recv()
            at = (order[1] * peers + peer_me) * n_group + h
            sums[at] = sums[at] + relay[h]

        pass_on(1, h, 2 - 2 * inner)

    def pass_third(h):
        add_pairs(2, h)
        pass_on(2, h, 1)

    def for_groups(step, action, start=0, stop=n_group):
        def one(i, c):
            action(turn(step, i))
            return c

        lax.fori_loop(start, stop, one, 0)

    @pl.when(inner == 0)
    def _():
        for g in range(n_group):
            recv[g * places + 2] = jnp.zeros(recv.shape[1:], jnp.float32)

    def open_up():
        pl.semaphore_wait(barrier, met)
        start_pairs(0)
        signal_near(near_sem)
        tables_load.start()
        rows_load.wait()

        def row_step(o, c):
            send_rows(lax.rem(group + o, n_group)).start()
            return c

        lax.fori_loop(1, n_group, row_step, 0)

    def meet_far():
        pl.semaphore_wait(near_sem, met)
        pl.semaphore_signal(
            far_sem, inc=1, device_id={"group": group, "local": near * peers + peer_me}, device_id_type=MESH
        )

        @pl.when(inner == 1)
        def _():
            pl.semaphore_signal(
                far_sem, inc=1, device_id={"group": group, "local": across * peers + peer_me}, device_id_type=MESH
            )

    def stay():
        def stay_step(h):
            pl.when(h != group)(lambda: send_bucket(local, h, 3 + peer_me).start())

        for_groups(3, stay_step)
        recv[group * places + 3 + peer_me] = sums[local * n_group + group]

    def own():
        def own_step(i, c):
            l = block_me * peers + lax.rem(peer_me + 1 + i // n_group, peers)
            send_bucket(l, turn(3, lax.rem(i, n_group)), 3 + peer_me).start()
            return c

        lax.fori_loop(0, (peers - 1) * n_group, own_step, 0)

    def relay_some(start, stop, late):
        pl.when(lax.rem(group, 2) != late)(lambda: for_groups(0, pass_first, start, stop))

    def add_runs(block, o, *actions):
        runs.append(whole(block, o))
        events[len(runs) - 1] = actions

    def add_peers(block, *actions):
        for o in range(1, peers):
            add_runs(block, o, *(actions if o == peers - 1 else ()))

    first_half, second_half = (0, early), (early, n_group)
    add_peers(order[0], open_up)
    add_runs(order[3], 0, stay)
    add_runs(order[0], 0)
    add_peers(order[1], lambda: start_pairs(1), meet_far, lambda: relay_some(*first_half, 0))
    add_runs(order[1], 0, lambda: relay_some(*second_half, 0), lambda: relay_some(*first_half, 1))
    add_peers(order[2], lambda: start_pairs(2))
    add_runs(order[2], 0, lambda: relay_some(*second_half, 1))
    add_peers(order[3], own)

    index_load.wait()
    grads_load.wait()

    def sum_step(q, c):
        sum_runs(q)
        for k, actions in events.items():

            @pl.when(q == k)
            def _():
                for action in actions:
                    action()

        return c

    lax.fori_loop(0, len(runs), sum_step, 0)

    pl.semaphore_wait(far_sem, 1 + inner)

    for_groups(1, pass_second)
    for_groups(2, pass_third)

    row_wait = pltpu.make_async_remote_copy(
        src_ref=rows_recv.at[pl.ds(0, n_group - 1)], dst_ref=rows_recv.at[pl.ds(0, n_group - 1)],
        send_sem=row_send_sem, recv_sem=row_recv_sem,
        device_id={"group": group, "local": local}, device_id_type=MESH,
    )
    rows_recv[group] = rows[...]
    row_wait.wait_recv()
    accums_load.wait()
    base = ((group * n_local + local) * rows_dev).astype(jnp.float32)
    slot_at = lax.broadcasted_iota(jnp.int32, (capacity, slots), 0)
    lane_at = lax.broadcasted_iota(jnp.int32, (capacity, slots), 1)
    first_at = lax.broadcasted_iota(jnp.int32, (slots, slots), 0)
    second_at = lax.broadcasted_iota(jnp.int32, (slots, slots), 1)
    row_lane = lax.broadcasted_iota(jnp.int32, (slots, rows_dev), 1).astype(jnp.float32)
    for t in range(2):
        columns = []
        for g in range(n_group):
            mine = lane_at == slot_at + group * capacity
            numbers = rows_recv[g, t : t + 1, :].astype(jnp.float32)
            columns.append(jnp.sum(jnp.where(mine, numbers, 0.0), axis=1, keepdims=True))
        column = jnp.concatenate(columns, axis=0)
        column = jnp.where(column < 0.0, -1.0, column - base)
        as_row = jnp.sum(jnp.where(first_at == second_at, column, 0.0), axis=0, keepdims=True)
        same = jnp.where(column == as_row, 1.0, 0.0)
        same_ref[t] = jnp.concatenate([same] * 3, axis=1).astype(jnp.bfloat16)
        hit = jnp.where(row_lane == column, 1.0, 0.0)
        hit_ref[t] = hit
        old_ref[t] = jnp.broadcast_to(jnp.sum(hit * accums[t : t + 1, :], axis=1, keepdims=True), old_ref.shape[1:])
        earlier = jnp.max(jnp.where(first_at < second_at, same, 0.0), axis=0, keepdims=True)
        target = jnp.where(earlier > 0.0, -1.0, as_row)
        target = jnp.concatenate([target] * 3, axis=1)
        piece = rows_dev // 8
        for i in range(8):
            piece_row = lax.broadcasted_iota(jnp.int32, (piece, 3 * slots), 0).astype(jnp.float32) + float(i * piece)
            onehot_ref[t, i * piece : (i + 1) * piece] = jnp.where(piece_row == target, 1.0, 0.0).astype(jnp.bfloat16)

    row_wait.wait_send()
    tables_load.wait()
    pair_parts = (BLOCKS - 1) * n_group * (peers - 1)
    pltpu.make_async_remote_copy(
        src_ref=pair.at[pl.ds(0, pair_parts)], dst_ref=pair.at[pl.ds(0, pair_parts)],
        send_sem=pair_send_sem, recv_sem=recv_sem,
        device_id={"group": group, "local": local}, device_id_type=MESH,
    ).wait_send()
    sent = (BLOCKS - 1) * n_group + buckets - 1
    pltpu.make_async_remote_copy(
        src_ref=sums.at[pl.ds(0, sent)], dst_ref=sums.at[pl.ds(0, sent)],
        send_sem=send_sem, recv_sem=recv_sem,
        device_id={"group": group, "local": local}, device_id_type=MESH,
    ).wait_send()
    def wait_parts(n):
        pltpu.make_async_remote_copy(
            src_ref=recv.at[pl.ds(0, n)], dst_ref=recv.at[pl.ds(0, n)],
            send_sem=send_sem, recv_sem=recv_sem,
            device_id={"group": group, "local": local}, device_id_type=MESH,
        ).wait_recv()

    pl.when(inner == 0)(lambda: wait_parts(n_group * (places - 1) - 1))
    pl.when(inner == 1)(lambda: wait_parts(n_group * places - 1))
    for t in range(2):
        lists = []
        for g in range(n_group):
            total = recv[g * places, t]
            for p in range(1, places):
                total = total + recv[g * places + p, t]
            lists.append(total)
        totals = jnp.dot(
            same_ref[t], split_bf16(jnp.concatenate(lists, axis=0)), preferred_element_type=jnp.float32
        )
        squares = jnp.mean(totals * totals, axis=1, keepdims=True)
        added = jnp.max(hit_ref[t] * squares, axis=0, keepdims=True)
        new_accums_ref[t : t + 1, :] = accums[t : t + 1, :] + added
        change = learning_rate * totals / (jnp.sqrt(old_ref[t][:, 0:1] + squares) + epsilon)
        parts_ref[t] = split_bf16(change)


def update_kernel(parts_ref, onehot_ref, tables_ref, accums_ref, new_tables_hbm, new_accums_hbm, new, out_sems, accums_sem):
    rows_dev = tables_ref.shape[1]
    piece = rows_dev // PIECES
    accums_out = pltpu.make_async_copy(accums_ref, new_accums_hbm, accums_sem)
    accums_out.start()

    def out(t, i):
        at = pl.ds(i * piece, piece)
        return pltpu.make_async_copy(new.at[t, at], new_tables_hbm.at[t, at], out_sems.at[t, i])

    def step(k, c):
        t, i = k // PIECES, lax.rem(k, PIECES)
        at = pl.ds(pl.multiple_of(i * piece, piece), piece)
        new[t, at] = tables_ref[t, at] - jnp.dot(onehot_ref[t, at], parts_ref[t], preferred_element_type=jnp.float32)
        out(t, i).start()
        return c

    lax.fori_loop(0, 2 * PIECES, step, 0)
    accums_out.wait()
    for t in range(2):
        for i in range(PIECES):
            out(t, i).wait()


def local_step(n_group, n_local, lookup_grads, slot_index, unique_rows, tables, accums):
    look, width = lookup_grads.shape
    slots = unique_rows.shape[1]
    capacity = slots // n_group
    n_dev = n_group * n_local
    rows_dev = tables.shape[1]
    peers = n_local // BLOCKS
    vmem = pl.BlockSpec(memory_space=pltpu.VMEM)
    hbm = pl.BlockSpec(memory_space=pltpu.HBM)
    dma = pltpu.SemaphoreType.DMA
    regular = pltpu.SemaphoreType.REGULAR
    prepared = pl.pallas_call(
        functools.partial(exchange_kernel, n_group, n_local),
        out_shape=(
            pltpu.VMEM((2, 3 * slots, width), jnp.bfloat16),
            pltpu.VMEM((2, rows_dev, 3 * slots), jnp.bfloat16),
            pltpu.VMEM(tables.shape, jnp.float32),
            pltpu.VMEM(accums.shape, jnp.float32),
        ),
        in_specs=[hbm] * 5,
        out_specs=(vmem, vmem, vmem, vmem),
        scratch_shapes=[
            pltpu.VMEM((look, width), jnp.bfloat16),
            pltpu.VMEM((2, look), jnp.int32),
            pltpu.VMEM((2, slots), jnp.int32),
            pltpu.VMEM((2, rows_dev), jnp.float32),
            pltpu.VMEM((n_dev, 2, capacity, width), jnp.float32),
            pltpu.VMEM(((BLOCKS - 1) * n_group * (peers - 1), 2, capacity, width), jnp.float32),
            pltpu.VMEM((n_group, 2, capacity, width), jnp.float32),
            pltpu.VMEM((n_group * (3 + peers), 2, capacity, width), jnp.float32),
            pltpu.VMEM((n_group, 2, slots), jnp.int32),
            pltpu.VMEM((2, slots, 3 * slots), jnp.bfloat16),
            pltpu.VMEM((2, slots, rows_dev), jnp.float32),
            pltpu.VMEM((2, slots, 128), jnp.float32),
            dma, dma, dma, dma, dma,
            dma(((BLOCKS - 1) * n_group,)), dma((n_group,)),
            dma, dma, dma, dma, dma, regular, regular,
        ],
        compiler_params=pltpu.CompilerParams(
            collective_id=0, has_side_effects=True, vmem_limit_bytes=48 * 2**20
        ),
        cost_estimate=pl.CostEstimate(flops=2 * 2 * look * width * slots * n_local, bytes_accessed=2 * look * width, transcendentals=0),
    )(*[pltpu.with_memory_space_constraint(x, pltpu.HBM) for x in (lookup_grads, slot_index, unique_rows, tables, accums)])
    return pl.pallas_call(
        update_kernel,
        out_shape=(
            jax.ShapeDtypeStruct(tables.shape, jnp.float32),
            jax.ShapeDtypeStruct(accums.shape, jnp.float32),
        ),
        in_specs=[vmem] * 4,
        out_specs=(hbm, hbm),
        scratch_shapes=[
            pltpu.VMEM((2, rows_dev, width), jnp.float32),
            dma((2, PIECES)), dma,
        ],
        compiler_params=pltpu.CompilerParams(vmem_limit_bytes=16 * 2**20),
    )(*prepared)


def solution(mesh):
    n_group, n_local = mesh.shape["group"], mesh.shape["local"]
    return jax.shard_map(
        functools.partial(local_step, n_group, n_local),
        mesh=mesh,
        in_specs=(
            P(("group", "local"), None),
            P(None, ("group", "local")),
            P(None, ("group", "local")),
            P(None, ("group", "local"), None),
            P(None, ("group", "local")),
        ),
        out_specs=(P(None, ("group", "local"), None), P(None, ("group", "local"))),
        check_vma=False,
    )
```

```python
import functools

import jax
import jax.numpy as jnp
from jax import lax
from jax.experimental import pallas as pl
from jax.experimental.pallas import tpu as pltpu
from jax.sharding import PartitionSpec as P

learning_rate = 0.1
epsilon = 1e-08
MESH = pl.DeviceIdType.MESH
PIECES = 4
BLOCKS = 4


def split_bf16(x):
    high = x.astype(jnp.bfloat16)
    rest = x - high.astype(jnp.float32)
    middle = rest.astype(jnp.bfloat16)
    low = (rest - middle.astype(jnp.float32)).astype(jnp.bfloat16)
    return jnp.concatenate([high, middle, low], axis=0)


def exchange_kernel(
    n_group, n_local, grads_hbm, index_hbm, rows_hbm, tables_hbm, accums_hbm,
    parts_ref, onehot_ref, tables_ref, new_accums_ref,
    grads, index, rows, accums, sums, pair, relay, raw, recv, rows_recv, same_ref, hit_ref, old_ref,
    grads_sems, index_sem, rows_sem, tables_sem, accums_sem, pair_sems, relay_sems, raw_sem,
    pair_send_sem, send_sem, recv_sem, row_send_sem, row_recv_sem, near_sem, far_sem,
):
    group, local = lax.axis_index("group"), lax.axis_index("local")
    width = grads.shape[1]
    capacity = sums.shape[2]
    slots = rows.shape[1]
    rows_dev = tables_hbm.shape[1]
    peers = n_local // BLOCKS
    buckets = peers * n_group
    early = n_group // 2
    places = 3 + peers
    block_me, peer_me = local // peers, lax.rem(local, peers)
    half = block_me // 2
    inner = lax.rem(block_me + half, 2)
    near = block_me + 1 - 2 * lax.rem(block_me, 2)
    across = BLOCKS - 1 - block_me
    far_inner, far_outer = 2 - half, BLOCKS - 1 - 3 * half
    order = (
        far_outer + inner * (far_inner - far_outer), far_inner + inner * (far_outer - far_inner), near, block_me
    )

    def signal_near(sem):
        for o in range(1, peers):
            pl.semaphore_signal(
                sem, inc=1, device_id={"group": group, "local": block_me * peers + lax.rem(peer_me + o, peers)},
                device_id_type=MESH,
            )
        pl.semaphore_signal(
            sem, inc=1, device_id={"group": group, "local": near * peers + peer_me}, device_id_type=MESH
        )

        @pl.when(inner == 1)
        def _():
            pl.semaphore_signal(
                sem, inc=1, device_id={"group": group, "local": across * peers + peer_me}, device_id_type=MESH
            )

        for o in range(1, n_group):
            pl.semaphore_signal(
                sem, inc=1, device_id={"group": lax.rem(group + o, n_group), "local": local}, device_id_type=MESH
            )

    met = peers - 1 + 1 + n_group - 1 + inner

    index_load = pltpu.make_async_copy(index_hbm, index, index_sem)
    rows_load = pltpu.make_async_copy(rows_hbm, rows, rows_sem)
    tables_load = pltpu.make_async_copy(tables_hbm, tables_ref, tables_sem)
    accums_load = pltpu.make_async_copy(accums_hbm, accums, accums_sem)

    look = grads.shape[0]
    halves_at = pl.ds(0, look // 2), pl.ds(look // 2, look - look // 2)
    grads_loads = [
        pltpu.make_async_copy(grads_hbm.at[at], grads.at[at], grads_sems.at[k]) for k, at in enumerate(halves_at)
    ]

    index_load.start()
    for grads_load in grads_loads:
        grads_load.start()
    rows_load.start()
    accums_load.start()
    barrier = pltpu.get_barrier_semaphore()
    signal_near(barrier)

    def send_pair(step, o, h):
        to = order[step] * peers + lax.rem(peer_me + o, peers)
        return pltpu.make_async_remote_copy(
            src_ref=sums.at[to * n_group + h],
            dst_ref=pair.at[(step * n_group + h) * (peers - 1) + (peers - 1 - o)],
            send_sem=pair_send_sem, recv_sem=pair_sems.at[step * n_group + h],
            device_id={"group": group, "local": block_me * peers + lax.rem(peer_me + o, peers)},
            device_id_type=MESH,
        )

    def send_relay(h):
        return pltpu.make_async_remote_copy(
            src_ref=sums.at[(order[0] * peers + peer_me) * n_group + h], dst_ref=relay.at[h],
            send_sem=send_sem, recv_sem=relay_sems.at[h],
            device_id={"group": group, "local": near * peers + peer_me}, device_id_type=MESH,
        )

    def send_bucket(l, h, place):
        return pltpu.make_async_remote_copy(
            src_ref=sums.at[l * n_group + h], dst_ref=recv.at[group * places + place],
            send_sem=send_sem, recv_sem=recv_sem,
            device_id={"group": h, "local": l}, device_id_type=MESH,
        )

    def send_rows(h):
        return pltpu.make_async_remote_copy(
            src_ref=rows, dst_ref=rows_recv.at[group],
            send_sem=row_send_sem, recv_sem=row_recv_sem,
            device_id={"group": h, "local": local}, device_id_type=MESH,
        )

    def whole(block, o):
        at = (block * peers + lax.rem(peer_me + o, peers)) * n_group
        return at, at + early

    def halves(p, h):
        at = (near * peers + p) * n_group + h
        return at, at + n_group

    runs, events = [], {}

    def sum_runs(q, cuts, ready=None):
        first, second = (
            functools.reduce(lambda x, k: jnp.where(q == k, runs[k][i], x), range(1, len(runs)), runs[0][i])
            for i in range(2)
        )
        n_rows = early * capacity
        row = lax.broadcasted_iota(jnp.int32, (n_rows, 1), 0)
        targets = jnp.concatenate([row + first * capacity, row + second * capacity], axis=0)
        total = None
        for k, at in enumerate(cuts):
            if ready is not None:
                ready[k].wait()
            onehot = jnp.concatenate(
                [jnp.where(index[t : t + 1, at] == targets, 1.0, 0.0).astype(jnp.bfloat16) for t in range(2)], axis=0
            )
            part = jnp.dot(onehot, grads[at, :], preferred_element_type=jnp.float32)
            total = part if total is None else total + part
        for t in range(2):
            for i, at in enumerate((first, second)):
                start = (2 * t + i) * n_rows
                sums[pl.ds(at, early), t] = total[start : start + n_rows, :].reshape(early, capacity, width)

    def start_pairs(step):
        def one(i, c):
            send_pair(step, 1 + i // n_group, lax.rem(i, n_group)).start()
            return c

        lax.fori_loop(0, (peers - 1) * n_group, one, 0)

    def start_third():
        def one(i, c):
            send_pair(2, 1 + i // early, lax.rem(i, early)).start()
            return c

        lax.fori_loop(0, (peers - 1) * early, one, 0)

    def send_raw():
        def one(p, c):
            pltpu.make_async_remote_copy(
                src_ref=sums.at[pl.ds((near * peers + p) * n_group + early, n_group - early)],
                dst_ref=raw.at[pl.ds(p * (n_group - early), n_group - early)],
                send_sem=send_sem, recv_sem=raw_sem,
                device_id={"group": group, "local": near * peers + peer_me}, device_id_type=MESH,
            ).start()
            return c

        lax.fori_loop(0, peers, one, 0)

    def add_raw():
        pltpu.make_async_remote_copy(
            src_ref=raw, dst_ref=raw, send_sem=send_sem, recv_sem=raw_sem,
            device_id={"group": group, "local": local}, device_id_type=MESH,
        ).wait_recv()

        def one(p, c):
            at = pl.ds((block_me * peers + p) * n_group + early, n_group - early)
            sums[at] = sums[at] + raw[pl.ds(p * (n_group - early), n_group - early)]
            return c

        lax.fori_loop(0, peers, one, 0)

    def add_pairs(step, h):
        first = (step * n_group + h) * (peers - 1)
        pltpu.make_async_remote_copy(
            src_ref=pair.at[pl.ds(first, peers - 1)], dst_ref=pair.at[pl.ds(first, peers - 1)],
            send_sem=pair_send_sem, recv_sem=pair_sems.at[step * n_group + h],
            device_id={"group": group, "local": local}, device_id_type=MESH,
        ).wait_recv()
        at = (order[step] * peers + peer_me) * n_group + h
        total = sums[at]
        for p in range(peers - 1):
            total = total + pair[first + p]
        sums[at] = total

    def pass_on(step, h, place):
        send_bucket(order[step] * peers + peer_me, h, place).start()

    def pass_first(h):
        add_pairs(0, h)
        pl.when(inner == 0)(lambda: send_relay(h).start())
        pl.when(inner == 1)(lambda: pass_on(0, h, 0))

    def pass_second(h):
        add_pairs(1, h)

        @pl.when(inner == 1)
        def _():
            pltpu.make_async_remote_copy(
                src_ref=relay.at[h], dst_ref=relay.at[h], send_sem=send_sem, recv_sem=relay_sems.at[h],
                device_id={"group": group, "local": local}, device_id_type=MESH,
            ).wait_recv()
            at = (order[1] * peers + peer_me) * n_group + h
            sums[at] = sums[at] + relay[h]

        pass_on(1, h, 2 - 2 * inner)

    def pass_third(h):
        add_pairs(2, h)
        pass_on(2, h, 1)

    def for_groups(action, start=0, stop=n_group):
        def one(h, c):
            action(h)
            return c

        lax.fori_loop(start, stop, one, 0)

    @pl.when(inner == 0)
    def _():
        for g in range(n_group):
            recv[g * places + 2] = jnp.zeros(recv.shape[1:], jnp.float32)

    @pl.when(group >= early)
    def _():
        for g in range(n_group):
            recv[g * places + 1] = jnp.zeros(recv.shape[1:], jnp.float32)

    def open_up():
        pl.semaphore_wait(barrier, met)
        start_pairs(0)
        signal_near(near_sem)
        tables_load.start()
        rows_load.wait()

        def row_step(o, c):
            send_rows(lax.rem(group + o, n_group)).start()
            return c

        lax.fori_loop(1, n_group, row_step, 0)

    def meet_far():
        pl.semaphore_wait(near_sem, met)
        pl.semaphore_signal(
            far_sem, inc=1, device_id={"group": group, "local": near * peers + peer_me}, device_id_type=MESH
        )

        @pl.when(inner == 1)
        def _():
            pl.semaphore_signal(
                far_sem, inc=1, device_id={"group": group, "local": across * peers + peer_me}, device_id_type=MESH
            )

    def stay(start, stop):
        def one(h, c):
            pl.when(h != group)(lambda: send_bucket(local, h, 3 + peer_me).start())
            return c

        lax.fori_loop(start, stop, one, 0)

        @pl.when((group >= start) & (group < stop))
        def _():
            recv[group * places + 3 + peer_me] = sums[local * n_group + group]

    def own(start, stop):
        def one(i, c):
            l = block_me * peers + lax.rem(peer_me + 1 + i // (stop - start), peers)
            send_bucket(l, start + lax.rem(i, stop - start), 3 + peer_me).start()
            return c

        lax.fori_loop(0, (peers - 1) * (stop - start), one, 0)

    def relay_some(start, stop, late):
        pl.when(lax.rem(group, 2) != late)(lambda: for_groups(pass_first, start, stop))

    def add_runs(run, *actions):
        runs.append(run)
        events[len(runs) - 1] = actions

    def add_peers(block, *actions):
        for o in range(1, peers):
            add_runs(whole(block, o), *(actions if o == peers - 1 else ()))

    def add_near(h, *actions):
        for p in range(0, peers, 2):
            add_runs(halves(p, h), *(actions if p == peers - 2 else ()))

    first_half, second_half = (0, early), (early, n_group)
    add_peers(order[0], open_up)
    add_near(early, send_raw)
    add_runs(whole(order[0], 0))
    add_peers(order[1], lambda: start_pairs(1), meet_far, lambda: relay_some(*first_half, 0))
    add_runs(whole(order[1], 0), lambda: relay_some(*second_half, 0), lambda: relay_some(*first_half, 1))
    add_near(0, start_third, lambda: relay_some(*second_half, 1))
    add_runs(whole(block_me, 0), lambda: stay(*first_half))
    add_peers(block_me, lambda: own(*first_half))

    def act(k):
        for action in events[k]:
            action()

    index_load.wait()
    sum_runs(0, halves_at, grads_loads)
    act(0)

    def sum_step(q, c):
        sum_runs(q, (pl.ds(0, look),))
        for k in range(1, len(runs)):
            if events[k]:
                pl.when(q == k)(functools.partial(act, k))
        return c

    lax.fori_loop(1, len(runs), sum_step, 0)

    add_raw()
    own(*second_half)
    stay(*second_half)
    pl.semaphore_wait(far_sem, 1 + inner)
    def late_step(k, c):
        pl.when(k != inner)(lambda: for_groups(pass_second))

        pl.when(k == inner)(lambda: for_groups(pass_third, 0, early))
        return c

    lax.fori_loop(0, 2, late_step, 0)

    row_wait = pltpu.make_async_remote_copy(
        src_ref=rows_recv.at[pl.ds(0, n_group - 1)], dst_ref=rows_recv.at[pl.ds(0, n_group - 1)],
        send_sem=row_send_sem, recv_sem=row_recv_sem,
        device_id={"group": group, "local": local}, device_id_type=MESH,
    )
    rows_recv[group] = rows[...]
    row_wait.wait_recv()
    accums_load.wait()
    base = ((group * n_local + local) * rows_dev).astype(jnp.float32)
    slot_at = lax.broadcasted_iota(jnp.int32, (capacity, slots), 0)
    lane_at = lax.broadcasted_iota(jnp.int32, (capacity, slots), 1)
    first_at = lax.broadcasted_iota(jnp.int32, (slots, slots), 0)
    second_at = lax.broadcasted_iota(jnp.int32, (slots, slots), 1)
    row_lane = lax.broadcasted_iota(jnp.int32, (slots, rows_dev), 1).astype(jnp.float32)
    for t in range(2):
        columns = []
        for g in range(n_group):
            mine = lane_at == slot_at + group * capacity
            numbers = rows_recv[g, t : t + 1, :].astype(jnp.float32)
            columns.append(jnp.sum(jnp.where(mine, numbers, 0.0), axis=1, keepdims=True))
        column = jnp.concatenate(columns, axis=0)
        column = jnp.where(column < 0.0, -1.0, column - base)
        as_row = jnp.sum(jnp.where(first_at == second_at, column, 0.0), axis=0, keepdims=True)
        same = jnp.where(column == as_row, 1.0, 0.0)
        same_ref[t] = jnp.concatenate([same] * 3, axis=1).astype(jnp.bfloat16)
        hit = jnp.where(row_lane == column, 1.0, 0.0)
        hit_ref[t] = hit
        old_ref[t] = jnp.broadcast_to(jnp.sum(hit * accums[t : t + 1, :], axis=1, keepdims=True), old_ref.shape[1:])
        earlier = jnp.max(jnp.where(first_at < second_at, same, 0.0), axis=0, keepdims=True)
        target = jnp.where(earlier > 0.0, -1.0, as_row)
        target = jnp.concatenate([target] * 3, axis=1)
        piece = rows_dev // 8
        for i in range(8):
            piece_row = lax.broadcasted_iota(jnp.int32, (piece, 3 * slots), 0).astype(jnp.float32) + float(i * piece)
            onehot_ref[t, i * piece : (i + 1) * piece] = jnp.where(piece_row == target, 1.0, 0.0).astype(jnp.bfloat16)

    row_wait.wait_send()
    tables_load.wait()
    pair_parts = (2 * n_group + early) * (peers - 1)
    pltpu.make_async_remote_copy(
        src_ref=pair.at[pl.ds(0, pair_parts)], dst_ref=pair.at[pl.ds(0, pair_parts)],
        send_sem=pair_send_sem, recv_sem=recv_sem,
        device_id={"group": group, "local": local}, device_id_type=MESH,
    ).wait_send()
    sent = 2 * n_group + early + peers * (n_group - early) + buckets - 1
    pltpu.make_async_remote_copy(
        src_ref=sums.at[pl.ds(0, sent)], dst_ref=sums.at[pl.ds(0, sent)],
        send_sem=send_sem, recv_sem=recv_sem,
        device_id={"group": group, "local": local}, device_id_type=MESH,
    ).wait_send()
    def wait_parts(n):
        pltpu.make_async_remote_copy(
            src_ref=recv.at[pl.ds(0, n)], dst_ref=recv.at[pl.ds(0, n)],
            send_sem=send_sem, recv_sem=recv_sem,
            device_id={"group": group, "local": local}, device_id_type=MESH,
        ).wait_recv()

    for deep in range(2):
        pl.when((inner == deep) & (group >= early))(lambda: wait_parts(n_group * (places - 2 + deep) - 1))
        pl.when((inner == deep) & (group < early))(lambda: wait_parts(n_group * (places - 1 + deep) - 1))
    for t in range(2):
        lists = []
        for g in range(n_group):
            total = recv[g * places, t]
            for p in range(1, places):
                total = total + recv[g * places + p, t]
            lists.append(total)
        totals = jnp.dot(
            same_ref[t], split_bf16(jnp.concatenate(lists, axis=0)), preferred_element_type=jnp.float32
        )
        squares = jnp.mean(totals * totals, axis=1, keepdims=True)
        added = jnp.max(hit_ref[t] * squares, axis=0, keepdims=True)
        new_accums_ref[t : t + 1, :] = accums[t : t + 1, :] + added
        change = learning_rate * totals / (jnp.sqrt(old_ref[t][:, 0:1] + squares) + epsilon)
        parts_ref[t] = split_bf16(change)


def update_kernel(parts_ref, onehot_ref, tables_ref, accums_ref, new_tables_hbm, new_accums_hbm, new, out_sems, accums_sem):
    rows_dev = tables_ref.shape[1]
    piece = rows_dev // PIECES
    accums_out = pltpu.make_async_copy(accums_ref, new_accums_hbm, accums_sem)
    accums_out.start()

    def out(t, i):
        at = pl.ds(i * piece, piece)
        return pltpu.make_async_copy(new.at[t, at], new_tables_hbm.at[t, at], out_sems.at[t, i])

    for t in range(2):
        for i in range(PIECES):
            at = slice(i * piece, (i + 1) * piece)
            new[t, at] = tables_ref[t, at] - jnp.dot(
                onehot_ref[t, at], parts_ref[t], preferred_element_type=jnp.float32
            )
            out(t, i).start()
    accums_out.wait()
    for t in range(2):
        for i in range(PIECES):
            out(t, i).wait()


def local_step(n_group, n_local, lookup_grads, slot_index, unique_rows, tables, accums):
    look, width = lookup_grads.shape
    slots = unique_rows.shape[1]
    capacity = slots // n_group
    n_dev = n_group * n_local
    rows_dev = tables.shape[1]
    peers = n_local // BLOCKS
    vmem = pl.BlockSpec(memory_space=pltpu.VMEM)
    hbm = pl.BlockSpec(memory_space=pltpu.HBM)
    dma = pltpu.SemaphoreType.DMA
    regular = pltpu.SemaphoreType.REGULAR
    prepared = pl.pallas_call(
        functools.partial(exchange_kernel, n_group, n_local),
        out_shape=(
            pltpu.VMEM((2, 3 * slots, width), jnp.bfloat16),
            pltpu.VMEM((2, rows_dev, 3 * slots), jnp.bfloat16),
            pltpu.VMEM(tables.shape, jnp.float32),
            pltpu.VMEM(accums.shape, jnp.float32),
        ),
        in_specs=[hbm] * 5,
        out_specs=(vmem, vmem, vmem, vmem),
        scratch_shapes=[
            pltpu.VMEM((look, width), jnp.bfloat16),
            pltpu.VMEM((2, look), jnp.int32),
            pltpu.VMEM((2, slots), jnp.int32),
            pltpu.VMEM((2, rows_dev), jnp.float32),
            pltpu.VMEM((n_dev, 2, capacity, width), jnp.float32),
            pltpu.VMEM(((BLOCKS - 1) * n_group * (peers - 1), 2, capacity, width), jnp.float32),
            pltpu.VMEM((n_group, 2, capacity, width), jnp.float32),
            pltpu.VMEM((peers * (n_group - n_group // 2), 2, capacity, width), jnp.float32),
            pltpu.VMEM((n_group * (3 + peers), 2, capacity, width), jnp.float32),
            pltpu.VMEM((n_group, 2, slots), jnp.int32),
            pltpu.VMEM((2, slots, 3 * slots), jnp.bfloat16),
            pltpu.VMEM((2, slots, rows_dev), jnp.float32),
            pltpu.VMEM((2, slots, 128), jnp.float32),
            dma((2,)), dma, dma, dma, dma,
            dma(((BLOCKS - 1) * n_group,)), dma((n_group,)), dma,
            dma, dma, dma, dma, dma, regular, regular,
        ],
        compiler_params=pltpu.CompilerParams(
            collective_id=0, has_side_effects=True, vmem_limit_bytes=48 * 2**20
        ),
        cost_estimate=pl.CostEstimate(flops=2 * 2 * look * width * slots * n_local, bytes_accessed=2 * look * width, transcendentals=0),
    )(*[pltpu.with_memory_space_constraint(x, pltpu.HBM) for x in (lookup_grads, slot_index, unique_rows, tables, accums)])
    return pl.pallas_call(
        update_kernel,
        out_shape=(
            jax.ShapeDtypeStruct(tables.shape, jnp.float32),
            jax.ShapeDtypeStruct(accums.shape, jnp.float32),
        ),
        in_specs=[vmem] * 4,
        out_specs=(hbm, hbm),
        scratch_shapes=[
            pltpu.VMEM((2, rows_dev, width), jnp.float32),
            dma((2, PIECES)), dma,
        ],
        compiler_params=pltpu.CompilerParams(vmem_limit_bytes=16 * 2**20),
    )(*prepared)


def solution(mesh):
    n_group, n_local = mesh.shape["group"], mesh.shape["local"]
    return jax.shard_map(
        functools.partial(local_step, n_group, n_local),
        mesh=mesh,
        in_specs=(
            P(("group", "local"), None),
            P(None, ("group", "local")),
            P(None, ("group", "local")),
            P(None, ("group", "local"), None),
            P(None, ("group", "local")),
        ),
        out_specs=(P(None, ("group", "local"), None), P(None, ("group", "local"))),
        check_vma=False,
    )
```

```python
import functools

import jax
import jax.numpy as jnp
from jax import lax
from jax.experimental import pallas as pl
from jax.experimental.pallas import tpu as pltpu
from jax.sharding import PartitionSpec as P

learning_rate = 0.1
epsilon = 1e-08
MESH = pl.DeviceIdType.MESH
PIECES = 4
BLOCKS = 4


def split_bf16(x):
    high = x.astype(jnp.bfloat16)
    rest = x - high.astype(jnp.float32)
    middle = rest.astype(jnp.bfloat16)
    low = (rest - middle.astype(jnp.float32)).astype(jnp.bfloat16)
    return jnp.concatenate([high, middle, low], axis=0)


def exchange_kernel(
    n_group, n_local, grads_hbm, index_hbm, rows_hbm, tables_hbm, accums_hbm,
    parts_ref, onehot_ref, tables_ref, new_accums_ref,
    grads, index, rows, accums, sums, pair, relay, raw, recv, rows_recv, acc, same_ref, hit_ref, old_ref,
    grads_sems, index_sem, rows_sem, tables_sem, accums_sem, pair_sems, relay_sems, raw_sem,
    pair_send_sem, send_sem, recv_sem, row_send_sem, row_recv_sem, near_sem, far_sem,
):
    group, local = lax.axis_index("group"), lax.axis_index("local")
    width = grads.shape[1]
    capacity = sums.shape[2]
    slots = rows.shape[1]
    rows_dev = tables_hbm.shape[1]
    peers = n_local // BLOCKS
    buckets = peers * n_group
    early = n_group // 2
    places = 3 + peers
    block_me, peer_me = local // peers, lax.rem(local, peers)
    half = block_me // 2
    inner = lax.rem(block_me + half, 2)
    near = block_me + 1 - 2 * lax.rem(block_me, 2)
    across = BLOCKS - 1 - block_me
    far_inner, far_outer = 2 - half, BLOCKS - 1 - 3 * half
    order = (
        far_outer + inner * (far_inner - far_outer), far_inner + inner * (far_outer - far_inner), near, block_me
    )

    def signal_near(sem):
        for o in range(1, peers):
            pl.semaphore_signal(
                sem, inc=1, device_id={"group": group, "local": block_me * peers + lax.rem(peer_me + o, peers)},
                device_id_type=MESH,
            )
        pl.semaphore_signal(
            sem, inc=1, device_id={"group": group, "local": near * peers + peer_me}, device_id_type=MESH
        )

        @pl.when(inner == 1)
        def _():
            pl.semaphore_signal(
                sem, inc=1, device_id={"group": group, "local": across * peers + peer_me}, device_id_type=MESH
            )

        for o in range(1, n_group):
            pl.semaphore_signal(
                sem, inc=1, device_id={"group": lax.rem(group + o, n_group), "local": local}, device_id_type=MESH
            )

    met = peers - 1 + 1 + n_group - 1 + inner

    index_load = pltpu.make_async_copy(index_hbm, index, index_sem)
    rows_load = pltpu.make_async_copy(rows_hbm, rows, rows_sem)
    tables_load = pltpu.make_async_copy(tables_hbm, tables_ref, tables_sem)
    accums_load = pltpu.make_async_copy(accums_hbm, accums, accums_sem)

    look = grads.shape[0]

    def load(k):
        at = pl.ds(pl.multiple_of(k * (look // 2), look // 2), look // 2)
        return pltpu.make_async_copy(grads_hbm.at[at], grads.at[at], grads_sems.at[k])

    index_load.start()
    for k in range(2):
        load(k).start()
    rows_load.start()
    accums_load.start()
    barrier = pltpu.get_barrier_semaphore()
    signal_near(barrier)

    def send_pair(step, o, h):
        to = order[step] * peers + lax.rem(peer_me + o, peers)
        return pltpu.make_async_remote_copy(
            src_ref=sums.at[to * n_group + h],
            dst_ref=pair.at[(step * n_group + h) * (peers - 1) + (peers - 1 - o)],
            send_sem=pair_send_sem, recv_sem=pair_sems.at[step * n_group + h],
            device_id={"group": group, "local": block_me * peers + lax.rem(peer_me + o, peers)},
            device_id_type=MESH,
        )

    def send_relay(h):
        return pltpu.make_async_remote_copy(
            src_ref=sums.at[(order[0] * peers + peer_me) * n_group + h], dst_ref=relay.at[h],
            send_sem=send_sem, recv_sem=relay_sems.at[h],
            device_id={"group": group, "local": near * peers + peer_me}, device_id_type=MESH,
        )

    def send_bucket(l, h, place):
        return pltpu.make_async_remote_copy(
            src_ref=sums.at[l * n_group + h], dst_ref=recv.at[group * places + place],
            send_sem=send_sem, recv_sem=recv_sem,
            device_id={"group": h, "local": l}, device_id_type=MESH,
        )

    def send_rows(h):
        return pltpu.make_async_remote_copy(
            src_ref=rows, dst_ref=rows_recv.at[group],
            send_sem=row_send_sem, recv_sem=row_recv_sem,
            device_id={"group": h, "local": local}, device_id_type=MESH,
        )

    def whole(block, o):
        at = (block * peers + lax.rem(peer_me + o, peers)) * n_group
        return at, at + early

    def halves(p, h):
        at = (near * peers + p) * n_group + h
        return at, at + n_group

    runs, events = [], {}

    def part_of(firsts, at):
        row = lax.broadcasted_iota(jnp.int32, (early * capacity, 1), 0)
        targets = jnp.concatenate([row + first * capacity for first in firsts], axis=0)
        onehot = jnp.concatenate(
            [jnp.where(index[t : t + 1, at] == targets, 1.0, 0.0).astype(jnp.bfloat16) for t in range(2)], axis=0
        )
        return jnp.dot(onehot, grads[at, :], preferred_element_type=jnp.float32)

    def keep(firsts, total):
        n_rows = early * capacity
        for t in range(2):
            for i, first in enumerate(firsts):
                start = (2 * t + i) * n_rows
                sums[pl.ds(first, early), t] = total[start : start + n_rows, :].reshape(early, capacity, width)

    def sum_runs(q):
        firsts = tuple(
            functools.reduce(lambda x, k: jnp.where(q == k, runs[k][i], x), range(1, len(runs)), runs[0][i])
            for i in range(2)
        )
        keep(firsts, part_of(firsts, pl.ds(0, look)))

    def sum_as_loaded(firsts):
        acc[...] = jnp.zeros_like(acc)

        def one(k, c):
            load(k).wait()
            acc[...] += part_of(firsts, pl.ds(pl.multiple_of(k * (look // 2), look // 2), look // 2))
            return c

        lax.fori_loop(0, 2, one, 0)
        keep(firsts, acc[...])

    def start_pairs(step):
        def one(i, c):
            send_pair(step, 1 + i // n_group, lax.rem(i, n_group)).start()
            return c

        lax.fori_loop(0, (peers - 1) * n_group, one, 0)

    def start_third():
        def one(i, c):
            send_pair(2, 1 + i // early, lax.rem(i, early)).start()
            return c

        lax.fori_loop(0, (peers - 1) * early, one, 0)

    def send_raw():
        def one(p, c):
            pltpu.make_async_remote_copy(
                src_ref=sums.at[pl.ds((near * peers + p) * n_group + early, n_group - early)],
                dst_ref=raw.at[pl.ds(p * (n_group - early), n_group - early)],
                send_sem=send_sem, recv_sem=raw_sem,
                device_id={"group": group, "local": near * peers + peer_me}, device_id_type=MESH,
            ).start()
            return c

        lax.fori_loop(0, peers, one, 0)

    def add_raw():
        pltpu.make_async_remote_copy(
            src_ref=raw, dst_ref=raw, send_sem=send_sem, recv_sem=raw_sem,
            device_id={"group": group, "local": local}, device_id_type=MESH,
        ).wait_recv()

        def one(p, c):
            at = pl.ds((block_me * peers + p) * n_group + early, n_group - early)
            sums[at] = sums[at] + raw[pl.ds(p * (n_group - early), n_group - early)]
            return c

        lax.fori_loop(0, peers, one, 0)

    def add_pairs(step, h):
        first = (step * n_group + h) * (peers - 1)
        pltpu.make_async_remote_copy(
            src_ref=pair.at[pl.ds(first, peers - 1)], dst_ref=pair.at[pl.ds(first, peers - 1)],
            send_sem=pair_send_sem, recv_sem=pair_sems.at[step * n_group + h],
            device_id={"group": group, "local": local}, device_id_type=MESH,
        ).wait_recv()
        at = (order[step] * peers + peer_me) * n_group + h
        total = sums[at]
        for p in range(peers - 1):
            total = total + pair[first + p]
        sums[at] = total

    def pass_on(step, h, place):
        send_bucket(order[step] * peers + peer_me, h, place).start()

    def pass_first(h):
        add_pairs(0, h)
        pl.when(inner == 0)(lambda: send_relay(h).start())
        pl.when(inner == 1)(lambda: pass_on(0, h, 0))

    def pass_second(h):
        add_pairs(1, h)

        @pl.when(inner == 1)
        def _():
            pltpu.make_async_remote_copy(
                src_ref=relay.at[h], dst_ref=relay.at[h], send_sem=send_sem, recv_sem=relay_sems.at[h],
                device_id={"group": group, "local": local}, device_id_type=MESH,
            ).wait_recv()
            at = (order[1] * peers + peer_me) * n_group + h
            sums[at] = sums[at] + relay[h]

        pass_on(1, h, 2 - 2 * inner)

    def pass_third(h):
        add_pairs(2, h)
        pass_on(2, h, 1)

    def for_groups(action, start=0, stop=n_group):
        def one(h, c):
            action(h)
            return c

        lax.fori_loop(start, stop, one, 0)

    @pl.when(inner == 0)
    def _():
        for g in range(n_group):
            recv[g * places + 2] = jnp.zeros(recv.shape[1:], jnp.float32)

    @pl.when(group >= early)
    def _():
        for g in range(n_group):
            recv[g * places + 1] = jnp.zeros(recv.shape[1:], jnp.float32)

    def open_up():
        pl.semaphore_wait(barrier, met)
        start_pairs(0)
        signal_near(near_sem)
        tables_load.start()
        rows_load.wait()

        def row_step(o, c):
            send_rows(lax.rem(group + o, n_group)).start()
            return c

        lax.fori_loop(1, n_group, row_step, 0)

    def meet_far():
        pl.semaphore_wait(near_sem, met)
        pl.semaphore_signal(
            far_sem, inc=1, device_id={"group": group, "local": near * peers + peer_me}, device_id_type=MESH
        )

        @pl.when(inner == 1)
        def _():
            pl.semaphore_signal(
                far_sem, inc=1, device_id={"group": group, "local": across * peers + peer_me}, device_id_type=MESH
            )

    def stay(start, stop):
        def one(h, c):
            pl.when(h != group)(lambda: send_bucket(local, h, 3 + peer_me).start())
            return c

        lax.fori_loop(start, stop, one, 0)

        @pl.when((group >= start) & (group < stop))
        def _():
            recv[group * places + 3 + peer_me] = sums[local * n_group + group]

    def own(start, stop):
        def one(i, c):
            l = block_me * peers + lax.rem(peer_me + 1 + i // (stop - start), peers)
            send_bucket(l, start + lax.rem(i, stop - start), 3 + peer_me).start()
            return c

        lax.fori_loop(0, (peers - 1) * (stop - start), one, 0)

    def relay_some(start, stop, late):
        pl.when(lax.rem(group, 2) != late)(lambda: for_groups(pass_first, start, stop))

    def add_runs(run, *actions):
        runs.append(run)
        events[len(runs) - 1] = actions

    def add_peers(block, *actions):
        for o in range(1, peers):
            add_runs(whole(block, o), *(actions if o == peers - 1 else ()))

    def add_near(h, *actions):
        for p in range(0, peers, 2):
            add_runs(halves(p, h), *(actions if p == peers - 2 else ()))

    first_half, second_half = (0, early), (early, n_group)
    add_peers(order[0], open_up)
    add_near(early, send_raw)
    add_runs(whole(order[0], 0))
    add_peers(order[1], lambda: start_pairs(1), meet_far, lambda: relay_some(*first_half, 0))
    add_runs(whole(order[1], 0), lambda: relay_some(*second_half, 0), lambda: relay_some(*first_half, 1))
    add_near(0, start_third, lambda: relay_some(*second_half, 1))
    add_runs(whole(block_me, 0), lambda: stay(*first_half))
    add_peers(block_me, lambda: own(*first_half))

    def act(k):
        for action in events[k]:
            action()

    index_load.wait()
    sum_as_loaded(runs[0])
    act(0)

    def sum_step(q, c):
        sum_runs(q)
        for k in range(1, len(runs)):
            if events[k]:
                pl.when(q == k)(functools.partial(act, k))
        return c

    lax.fori_loop(1, len(runs), sum_step, 0)

    add_raw()
    own(*second_half)
    stay(*second_half)
    pl.semaphore_wait(far_sem, 1 + inner)
    def late_step(k, c):
        pl.when(k != inner)(lambda: for_groups(pass_second))

        pl.when(k == inner)(lambda: for_groups(pass_third, 0, early))
        return c

    lax.fori_loop(0, 2, late_step, 0)

    row_wait = pltpu.make_async_remote_copy(
        src_ref=rows_recv.at[pl.ds(0, n_group - 1)], dst_ref=rows_recv.at[pl.ds(0, n_group - 1)],
        send_sem=row_send_sem, recv_sem=row_recv_sem,
        device_id={"group": group, "local": local}, device_id_type=MESH,
    )
    rows_recv[group] = rows[...]
    row_wait.wait_recv()
    accums_load.wait()
    base = ((group * n_local + local) * rows_dev).astype(jnp.float32)
    slot_at = lax.broadcasted_iota(jnp.int32, (capacity, slots), 0)
    lane_at = lax.broadcasted_iota(jnp.int32, (capacity, slots), 1)
    first_at = lax.broadcasted_iota(jnp.int32, (slots, slots), 0)
    second_at = lax.broadcasted_iota(jnp.int32, (slots, slots), 1)
    row_lane = lax.broadcasted_iota(jnp.int32, (slots, rows_dev), 1).astype(jnp.float32)
    for t in range(2):
        columns = []
        for g in range(n_group):
            mine = lane_at == slot_at + group * capacity
            numbers = rows_recv[g, t : t + 1, :].astype(jnp.float32)
            columns.append(jnp.sum(jnp.where(mine, numbers, 0.0), axis=1, keepdims=True))
        column = jnp.concatenate(columns, axis=0)
        column = jnp.where(column < 0.0, -1.0, column - base)
        as_row = jnp.sum(jnp.where(first_at == second_at, column, 0.0), axis=0, keepdims=True)
        same = jnp.where(column == as_row, 1.0, 0.0)
        same_ref[t] = jnp.concatenate([same] * 3, axis=1).astype(jnp.bfloat16)
        hit = jnp.where(row_lane == column, 1.0, 0.0)
        hit_ref[t] = hit
        old_ref[t] = jnp.broadcast_to(jnp.sum(hit * accums[t : t + 1, :], axis=1, keepdims=True), old_ref.shape[1:])
        earlier = jnp.max(jnp.where(first_at < second_at, same, 0.0), axis=0, keepdims=True)
        target = jnp.where(earlier > 0.0, -1.0, as_row)
        target = jnp.concatenate([target] * 3, axis=1)
        piece = rows_dev // 8
        for i in range(8):
            piece_row = lax.broadcasted_iota(jnp.int32, (piece, 3 * slots), 0).astype(jnp.float32) + float(i * piece)
            onehot_ref[t, i * piece : (i + 1) * piece] = jnp.where(piece_row == target, 1.0, 0.0).astype(jnp.bfloat16)

    row_wait.wait_send()
    tables_load.wait()
    pair_parts = (2 * n_group + early) * (peers - 1)
    pltpu.make_async_remote_copy(
        src_ref=pair.at[pl.ds(0, pair_parts)], dst_ref=pair.at[pl.ds(0, pair_parts)],
        send_sem=pair_send_sem, recv_sem=recv_sem,
        device_id={"group": group, "local": local}, device_id_type=MESH,
    ).wait_send()
    sent = 2 * n_group + early + peers * (n_group - early) + buckets - 1
    pltpu.make_async_remote_copy(
        src_ref=sums.at[pl.ds(0, sent)], dst_ref=sums.at[pl.ds(0, sent)],
        send_sem=send_sem, recv_sem=recv_sem,
        device_id={"group": group, "local": local}, device_id_type=MESH,
    ).wait_send()
    def wait_parts(n):
        pltpu.make_async_remote_copy(
            src_ref=recv.at[pl.ds(0, n)], dst_ref=recv.at[pl.ds(0, n)],
            send_sem=send_sem, recv_sem=recv_sem,
            device_id={"group": group, "local": local}, device_id_type=MESH,
        ).wait_recv()

    for deep in range(2):
        pl.when((inner == deep) & (group >= early))(lambda: wait_parts(n_group * (places - 2 + deep) - 1))
        pl.when((inner == deep) & (group < early))(lambda: wait_parts(n_group * (places - 1 + deep) - 1))
    for t in range(2):
        lists = []
        for g in range(n_group):
            total = recv[g * places, t]
            for p in range(1, places):
                total = total + recv[g * places + p, t]
            lists.append(total)
        totals = jnp.dot(
            same_ref[t], split_bf16(jnp.concatenate(lists, axis=0)), preferred_element_type=jnp.float32
        )
        squares = jnp.mean(totals * totals, axis=1, keepdims=True)
        added = jnp.max(hit_ref[t] * squares, axis=0, keepdims=True)
        new_accums_ref[t : t + 1, :] = accums[t : t + 1, :] + added
        change = learning_rate * totals / (jnp.sqrt(old_ref[t][:, 0:1] + squares) + epsilon)
        parts_ref[t] = split_bf16(change)


def update_kernel(parts_ref, onehot_ref, tables_ref, accums_ref, new_tables_hbm, new_accums_hbm, new, out_sems, accums_sem):
    rows_dev = tables_ref.shape[1]
    piece = rows_dev // PIECES
    accums_out = pltpu.make_async_copy(accums_ref, new_accums_hbm, accums_sem)
    accums_out.start()

    def out(t, i):
        at = pl.ds(i * piece, piece)
        return pltpu.make_async_copy(new.at[t, at], new_tables_hbm.at[t, at], out_sems.at[t, i])

    for t in range(2):
        for i in range(PIECES):
            at = slice(i * piece, (i + 1) * piece)
            new[t, at] = tables_ref[t, at] - jnp.dot(
                onehot_ref[t, at], parts_ref[t], preferred_element_type=jnp.float32
            )
            out(t, i).start()
    accums_out.wait()
    for t in range(2):
        for i in range(PIECES):
            out(t, i).wait()


def local_step(n_group, n_local, lookup_grads, slot_index, unique_rows, tables, accums):
    look, width = lookup_grads.shape
    slots = unique_rows.shape[1]
    capacity = slots // n_group
    n_dev = n_group * n_local
    rows_dev = tables.shape[1]
    peers = n_local // BLOCKS
    vmem = pl.BlockSpec(memory_space=pltpu.VMEM)
    hbm = pl.BlockSpec(memory_space=pltpu.HBM)
    dma = pltpu.SemaphoreType.DMA
    regular = pltpu.SemaphoreType.REGULAR
    prepared = pl.pallas_call(
        functools.partial(exchange_kernel, n_group, n_local),
        out_shape=(
            pltpu.VMEM((2, 3 * slots, width), jnp.bfloat16),
            pltpu.VMEM((2, rows_dev, 3 * slots), jnp.bfloat16),
            pltpu.VMEM(tables.shape, jnp.float32),
            pltpu.VMEM(accums.shape, jnp.float32),
        ),
        in_specs=[hbm] * 5,
        out_specs=(vmem, vmem, vmem, vmem),
        scratch_shapes=[
            pltpu.VMEM((look, width), jnp.bfloat16),
            pltpu.VMEM((2, look), jnp.int32),
            pltpu.VMEM((2, slots), jnp.int32),
            pltpu.VMEM((2, rows_dev), jnp.float32),
            pltpu.VMEM((n_dev, 2, capacity, width), jnp.float32),
            pltpu.VMEM(((BLOCKS - 1) * n_group * (peers - 1), 2, capacity, width), jnp.float32),
            pltpu.VMEM((n_group, 2, capacity, width), jnp.float32),
            pltpu.VMEM((peers * (n_group - n_group // 2), 2, capacity, width), jnp.float32),
            pltpu.VMEM((n_group * (3 + peers), 2, capacity, width), jnp.float32),
            pltpu.VMEM((n_group, 2, slots), jnp.int32),
            pltpu.VMEM((4 * (n_group // 2) * capacity, width), jnp.float32),
            pltpu.VMEM((2, slots, 3 * slots), jnp.bfloat16),
            pltpu.VMEM((2, slots, rows_dev), jnp.float32),
            pltpu.VMEM((2, slots, 128), jnp.float32),
            dma((2,)), dma, dma, dma, dma,
            dma(((BLOCKS - 1) * n_group,)), dma((n_group,)), dma,
            dma, dma, dma, dma, dma, regular, regular,
        ],
        compiler_params=pltpu.CompilerParams(
            collective_id=0, has_side_effects=True, vmem_limit_bytes=48 * 2**20
        ),
        cost_estimate=pl.CostEstimate(flops=2 * 2 * look * width * slots * n_local, bytes_accessed=2 * look * width, transcendentals=0),
    )(*[pltpu.with_memory_space_constraint(x, pltpu.HBM) for x in (lookup_grads, slot_index, unique_rows, tables, accums)])
    return pl.pallas_call(
        update_kernel,
        out_shape=(
            jax.ShapeDtypeStruct(tables.shape, jnp.float32),
            jax.ShapeDtypeStruct(accums.shape, jnp.float32),
        ),
        in_specs=[vmem] * 4,
        out_specs=(hbm, hbm),
        scratch_shapes=[
            pltpu.VMEM((2, rows_dev, width), jnp.float32),
            dma((2, PIECES)), dma,
        ],
        compiler_params=pltpu.CompilerParams(vmem_limit_bytes=16 * 2**20),
    )(*prepared)


def solution(mesh):
    n_group, n_local = mesh.shape["group"], mesh.shape["local"]
    return jax.shard_map(
        functools.partial(local_step, n_group, n_local),
        mesh=mesh,
        in_specs=(
            P(("group", "local"), None),
            P(None, ("group", "local")),
            P(None, ("group", "local")),
            P(None, ("group", "local"), None),
            P(None, ("group", "local")),
        ),
        out_specs=(P(None, ("group", "local"), None), P(None, ("group", "local"))),
        check_vma=False,
    )
```

```python
import functools

import jax
import jax.numpy as jnp
from jax import lax
from jax.experimental import pallas as pl
from jax.experimental.pallas import tpu as pltpu
from jax.sharding import PartitionSpec as P

learning_rate = 0.1
epsilon = 1e-08
MESH = pl.DeviceIdType.MESH
PIECES = 4
BLOCKS = 4


def split_bf16(x):
    high = x.astype(jnp.bfloat16)
    rest = x - high.astype(jnp.float32)
    middle = rest.astype(jnp.bfloat16)
    low = (rest - middle.astype(jnp.float32)).astype(jnp.bfloat16)
    return jnp.concatenate([high, middle, low], axis=0)


def exchange_kernel(
    n_group, n_local, grads_hbm, index_hbm, rows_hbm, tables_hbm, accums_hbm,
    parts_ref, onehot_ref, tables_ref, new_accums_ref,
    grads, index, rows, accums, sums, pair, relay, raw, recv, rows_recv, acc, same_ref, hit_ref, old_ref,
    grads_sems, index_sem, rows_sem, tables_sem, accums_sem, pair_sems, relay_sems, raw_sem,
    pair_send_sem, send_sem, recv_sem, row_send_sem, row_recv_sem, near_sem, far_sem,
):
    group, local = lax.axis_index("group"), lax.axis_index("local")
    width = grads.shape[1]
    capacity = sums.shape[2]
    slots = rows.shape[1]
    rows_dev = tables_hbm.shape[1]
    peers = n_local // BLOCKS
    buckets = peers * n_group
    early = n_group // 2
    places = 3 + peers
    block_me, peer_me = local // peers, lax.rem(local, peers)
    half = block_me // 2
    inner = lax.rem(block_me + half, 2)
    near = block_me + 1 - 2 * lax.rem(block_me, 2)
    across = BLOCKS - 1 - block_me
    far_inner, far_outer = 2 - half, BLOCKS - 1 - 3 * half
    order = (
        far_outer + inner * (far_inner - far_outer), far_inner + inner * (far_outer - far_inner), near, block_me
    )

    def signal_near(sem):
        for o in range(1, peers):
            pl.semaphore_signal(
                sem, inc=1, device_id={"group": group, "local": block_me * peers + lax.rem(peer_me + o, peers)},
                device_id_type=MESH,
            )
        pl.semaphore_signal(
            sem, inc=1, device_id={"group": group, "local": near * peers + peer_me}, device_id_type=MESH
        )

        @pl.when(inner == 1)
        def _():
            pl.semaphore_signal(
                sem, inc=1, device_id={"group": group, "local": across * peers + peer_me}, device_id_type=MESH
            )

        for o in range(1, n_group):
            pl.semaphore_signal(
                sem, inc=1, device_id={"group": lax.rem(group + o, n_group), "local": local}, device_id_type=MESH
            )

    met = peers - 1 + 1 + n_group - 1 + inner

    index_load = pltpu.make_async_copy(index_hbm, index, index_sem)
    rows_load = pltpu.make_async_copy(rows_hbm, rows, rows_sem)
    tables_load = pltpu.make_async_copy(tables_hbm, tables_ref, tables_sem)
    accums_load = pltpu.make_async_copy(accums_hbm, accums, accums_sem)

    look = grads.shape[0]

    def load(k):
        at = pl.ds(pl.multiple_of(k * (look // 2), look // 2), look // 2)
        return pltpu.make_async_copy(grads_hbm.at[at], grads.at[at], grads_sems.at[k])

    index_load.start()
    for k in range(2):
        load(k).start()
    rows_load.start()
    accums_load.start()
    barrier = pltpu.get_barrier_semaphore()
    signal_near(barrier)

    def send_pair(step, o, h):
        to = order[step] * peers + lax.rem(peer_me + o, peers)
        return pltpu.make_async_remote_copy(
            src_ref=sums.at[to * n_group + h],
            dst_ref=pair.at[(step * n_group + h) * (peers - 1) + (peers - 1 - o)],
            send_sem=pair_send_sem, recv_sem=pair_sems.at[step * n_group + h],
            device_id={"group": group, "local": block_me * peers + lax.rem(peer_me + o, peers)},
            device_id_type=MESH,
        )

    def send_relay(h):
        return pltpu.make_async_remote_copy(
            src_ref=sums.at[(order[0] * peers + peer_me) * n_group + h], dst_ref=relay.at[h],
            send_sem=send_sem, recv_sem=relay_sems.at[h],
            device_id={"group": group, "local": near * peers + peer_me}, device_id_type=MESH,
        )

    def send_bucket(l, h, place):
        return pltpu.make_async_remote_copy(
            src_ref=sums.at[l * n_group + h], dst_ref=recv.at[group * places + place],
            send_sem=send_sem, recv_sem=recv_sem,
            device_id={"group": h, "local": l}, device_id_type=MESH,
        )

    def send_rows(h):
        return pltpu.make_async_remote_copy(
            src_ref=rows, dst_ref=rows_recv.at[group],
            send_sem=row_send_sem, recv_sem=row_recv_sem,
            device_id={"group": h, "local": local}, device_id_type=MESH,
        )

    def whole(block, o):
        at = (block * peers + lax.rem(peer_me + o, peers)) * n_group
        return at, at + early

    def halves(p, h):
        at = (near * peers + p) * n_group + h
        return at, at + n_group

    runs, events = [], {}

    def part_of(firsts, at):
        row = lax.broadcasted_iota(jnp.int32, (early * capacity, 1), 0)
        targets = jnp.concatenate([row + first * capacity for first in firsts], axis=0)
        onehot = jnp.concatenate(
            [jnp.where(index[t : t + 1, at] == targets, 1.0, 0.0).astype(jnp.bfloat16) for t in range(2)], axis=0
        )
        return jnp.dot(onehot, grads[at, :], preferred_element_type=jnp.float32)

    def keep(firsts, total):
        n_rows = early * capacity
        for t in range(2):
            for i, first in enumerate(firsts):
                start = (2 * t + i) * n_rows
                sums[pl.ds(first, early), t] = total[start : start + n_rows, :].reshape(early, capacity, width)

    def sum_runs(q):
        firsts = tuple(
            functools.reduce(lambda x, k: jnp.where(q == k, runs[k][i], x), range(1, len(runs)), runs[0][i])
            for i in range(2)
        )
        keep(firsts, part_of(firsts, pl.ds(0, look)))

    def sum_as_loaded(firsts):
        acc[...] = jnp.zeros_like(acc)

        def one(k, c):
            load(k).wait()
            acc[...] += part_of(firsts, pl.ds(pl.multiple_of(k * (look // 2), look // 2), look // 2))
            return c

        lax.fori_loop(0, 2, one, 0)
        keep(firsts, acc[...])

    def start_pairs(step):
        def one(i, c):
            send_pair(step, 1 + i // n_group, lax.rem(i, n_group)).start()
            return c

        lax.fori_loop(0, (peers - 1) * n_group, one, 0)

    def start_third():
        def one(i, c):
            send_pair(2, 1 + i // early, lax.rem(i, early)).start()
            return c

        lax.fori_loop(0, (peers - 1) * early, one, 0)

    def send_raw():
        def one(p, c):
            pltpu.make_async_remote_copy(
                src_ref=sums.at[pl.ds((near * peers + p) * n_group + early, n_group - early)],
                dst_ref=raw.at[pl.ds(p * (n_group - early), n_group - early)],
                send_sem=send_sem, recv_sem=raw_sem,
                device_id={"group": group, "local": near * peers + peer_me}, device_id_type=MESH,
            ).start()
            return c

        lax.fori_loop(0, peers, one, 0)

    def add_raw():
        pltpu.make_async_remote_copy(
            src_ref=raw, dst_ref=raw, send_sem=send_sem, recv_sem=raw_sem,
            device_id={"group": group, "local": local}, device_id_type=MESH,
        ).wait_recv()

        def one(p, c):
            at = pl.ds((block_me * peers + p) * n_group + early, n_group - early)
            sums[at] = sums[at] + raw[pl.ds(p * (n_group - early), n_group - early)]
            return c

        lax.fori_loop(0, peers, one, 0)

    def add_pairs(step, h):
        first = (step * n_group + h) * (peers - 1)
        pltpu.make_async_remote_copy(
            src_ref=pair.at[pl.ds(first, peers - 1)], dst_ref=pair.at[pl.ds(first, peers - 1)],
            send_sem=pair_send_sem, recv_sem=pair_sems.at[step * n_group + h],
            device_id={"group": group, "local": local}, device_id_type=MESH,
        ).wait_recv()
        at = (order[step] * peers + peer_me) * n_group + h
        total = sums[at]
        for p in range(peers - 1):
            total = total + pair[first + p]
        sums[at] = total

    def pass_on(step, h, place):
        send_bucket(order[step] * peers + peer_me, h, place).start()

    def pass_first(h):
        add_pairs(0, h)
        pl.when(inner == 0)(lambda: send_relay(h).start())
        pl.when(inner == 1)(lambda: pass_on(0, h, 0))

    def pass_second(h):
        add_pairs(1, h)

        @pl.when(inner == 1)
        def _():
            pltpu.make_async_remote_copy(
                src_ref=relay.at[h], dst_ref=relay.at[h], send_sem=send_sem, recv_sem=relay_sems.at[h],
                device_id={"group": group, "local": local}, device_id_type=MESH,
            ).wait_recv()
            at = (order[1] * peers + peer_me) * n_group + h
            sums[at] = sums[at] + relay[h]

        pass_on(1, h, 2 - 2 * inner)

    def pass_third(h):
        add_pairs(2, h)
        pass_on(2, h, 1)

    def for_groups(action, start=0, stop=n_group):
        def one(h, c):
            action(h)
            return c

        lax.fori_loop(start, stop, one, 0)

    @pl.when(inner == 0)
    def _():
        for g in range(n_group):
            recv[g * places + 2] = jnp.zeros(recv.shape[1:], jnp.float32)

    @pl.when(group >= early)
    def _():
        for g in range(n_group):
            recv[g * places + 1] = jnp.zeros(recv.shape[1:], jnp.float32)

    def open_up():
        pl.semaphore_wait(barrier, met)
        start_pairs(0)
        signal_near(near_sem)
        tables_load.start()
        rows_load.wait()

        def row_step(o, c):
            send_rows(lax.rem(group + o, n_group)).start()
            return c

        lax.fori_loop(1, n_group, row_step, 0)

    def meet_far():
        pl.semaphore_wait(near_sem, met)
        pl.semaphore_signal(
            far_sem, inc=1, device_id={"group": group, "local": near * peers + peer_me}, device_id_type=MESH
        )

        @pl.when(inner == 1)
        def _():
            pl.semaphore_signal(
                far_sem, inc=1, device_id={"group": group, "local": across * peers + peer_me}, device_id_type=MESH
            )

    def stay(start, stop):
        def one(h, c):
            pl.when(h != group)(lambda: send_bucket(local, h, 3 + peer_me).start())
            return c

        lax.fori_loop(start, stop, one, 0)

        @pl.when((group >= start) & (group < stop))
        def _():
            recv[group * places + 3 + peer_me] = sums[local * n_group + group]

    def own(start, stop):
        def one(i, c):
            l = block_me * peers + lax.rem(peer_me + 1 + i // (stop - start), peers)
            send_bucket(l, start + lax.rem(i, stop - start), 3 + peer_me).start()
            return c

        lax.fori_loop(0, (peers - 1) * (stop - start), one, 0)

    def relay_some(start, stop, late):
        pl.when(lax.rem(group, 2) != late)(lambda: for_groups(pass_first, start, stop))

    def add_runs(run, *actions):
        runs.append(run)
        events[len(runs) - 1] = actions

    def add_peers(block, *actions):
        for o in range(1, peers):
            add_runs(whole(block, o), *(actions if o == peers - 1 else ()))

    def add_near(h, *actions):
        for p in range(0, peers, 2):
            add_runs(halves(p, h), *(actions if p == peers - 2 else ()))

    first_half, second_half = (0, early), (early, n_group)
    add_peers(order[0], open_up)
    add_near(early, send_raw)
    add_runs(whole(order[0], 0))
    add_peers(order[1], lambda: start_pairs(1), meet_far, lambda: relay_some(*first_half, 0))
    add_runs(whole(order[1], 0), lambda: relay_some(*second_half, 0), lambda: relay_some(*first_half, 1))
    add_near(0, start_third, lambda: relay_some(*second_half, 1))
    add_runs(whole(block_me, 0), lambda: stay(*first_half))
    add_peers(block_me, lambda: own(*first_half))

    def act(k):
        for action in events[k]:
            action()

    index_load.wait()
    sum_as_loaded(runs[0])
    act(0)

    def sum_step(q, c):
        sum_runs(q)
        for k in range(1, len(runs)):
            if events[k]:
                pl.when(q == k)(functools.partial(act, k))
        return c

    lax.fori_loop(1, len(runs), sum_step, 0)

    add_raw()
    own(*second_half)
    stay(*second_half)
    pl.semaphore_wait(far_sem, 1 + inner)
    second_first = jnp.maximum(inner, 1 - lax.rem(group, 2))

    def late_step(k, c):
        pl.when(k != second_first)(lambda: for_groups(pass_second))

        pl.when(k == second_first)(lambda: for_groups(pass_third, 0, early))
        return c

    lax.fori_loop(0, 2, late_step, 0)

    row_wait = pltpu.make_async_remote_copy(
        src_ref=rows_recv.at[pl.ds(0, n_group - 1)], dst_ref=rows_recv.at[pl.ds(0, n_group - 1)],
        send_sem=row_send_sem, recv_sem=row_recv_sem,
        device_id={"group": group, "local": local}, device_id_type=MESH,
    )
    rows_recv[group] = rows[...]
    row_wait.wait_recv()
    accums_load.wait()
    base = ((group * n_local + local) * rows_dev).astype(jnp.float32)
    slot_at = lax.broadcasted_iota(jnp.int32, (capacity, slots), 0)
    lane_at = lax.broadcasted_iota(jnp.int32, (capacity, slots), 1)
    first_at = lax.broadcasted_iota(jnp.int32, (slots, slots), 0)
    second_at = lax.broadcasted_iota(jnp.int32, (slots, slots), 1)
    row_lane = lax.broadcasted_iota(jnp.int32, (slots, rows_dev), 1).astype(jnp.float32)
    for t in range(2):
        columns = []
        for g in range(n_group):
            mine = lane_at == slot_at + group * capacity
            numbers = rows_recv[g, t : t + 1, :].astype(jnp.float32)
            columns.append(jnp.sum(jnp.where(mine, numbers, 0.0), axis=1, keepdims=True))
        column = jnp.concatenate(columns, axis=0)
        column = jnp.where(column < 0.0, -1.0, column - base)
        as_row = jnp.sum(jnp.where(first_at == second_at, column, 0.0), axis=0, keepdims=True)
        same = jnp.where(column == as_row, 1.0, 0.0)
        same_ref[t] = jnp.concatenate([same] * 3, axis=1).astype(jnp.bfloat16)
        hit = jnp.where(row_lane == column, 1.0, 0.0)
        hit_ref[t] = hit
        old_ref[t] = jnp.broadcast_to(jnp.sum(hit * accums[t : t + 1, :], axis=1, keepdims=True), old_ref.shape[1:])
        earlier = jnp.max(jnp.where(first_at < second_at, same, 0.0), axis=0, keepdims=True)
        target = jnp.where(earlier > 0.0, -1.0, as_row)
        target = jnp.concatenate([target] * 3, axis=1)
        piece = rows_dev // 8
        for i in range(8):
            piece_row = lax.broadcasted_iota(jnp.int32, (piece, 3 * slots), 0).astype(jnp.float32) + float(i * piece)
            onehot_ref[t, i * piece : (i + 1) * piece] = jnp.where(piece_row == target, 1.0, 0.0).astype(jnp.bfloat16)

    row_wait.wait_send()
    tables_load.wait()
    pair_parts = (2 * n_group + early) * (peers - 1)
    pltpu.make_async_remote_copy(
        src_ref=pair.at[pl.ds(0, pair_parts)], dst_ref=pair.at[pl.ds(0, pair_parts)],
        send_sem=pair_send_sem, recv_sem=recv_sem,
        device_id={"group": group, "local": local}, device_id_type=MESH,
    ).wait_send()
    sent = 2 * n_group + early + peers * (n_group - early) + buckets - 1
    pltpu.make_async_remote_copy(
        src_ref=sums.at[pl.ds(0, sent)], dst_ref=sums.at[pl.ds(0, sent)],
        send_sem=send_sem, recv_sem=recv_sem,
        device_id={"group": group, "local": local}, device_id_type=MESH,
    ).wait_send()
    def wait_parts(n):
        pltpu.make_async_remote_copy(
            src_ref=recv.at[pl.ds(0, n)], dst_ref=recv.at[pl.ds(0, n)],
            send_sem=send_sem, recv_sem=recv_sem,
            device_id={"group": group, "local": local}, device_id_type=MESH,
        ).wait_recv()

    for deep in range(2):
        pl.when((inner == deep) & (group >= early))(lambda: wait_parts(n_group * (places - 2 + deep) - 1))
        pl.when((inner == deep) & (group < early))(lambda: wait_parts(n_group * (places - 1 + deep) - 1))
    for t in range(2):
        lists = []
        for g in range(n_group):
            total = recv[g * places, t]
            for p in range(1, places):
                total = total + recv[g * places + p, t]
            lists.append(total)
        totals = jnp.dot(
            same_ref[t], split_bf16(jnp.concatenate(lists, axis=0)), preferred_element_type=jnp.float32
        )
        squares = jnp.mean(totals * totals, axis=1, keepdims=True)
        added = jnp.max(hit_ref[t] * squares, axis=0, keepdims=True)
        new_accums_ref[t : t + 1, :] = accums[t : t + 1, :] + added
        change = learning_rate * totals / (jnp.sqrt(old_ref[t][:, 0:1] + squares) + epsilon)
        parts_ref[t] = split_bf16(change)


def update_kernel(parts_ref, onehot_ref, tables_ref, accums_ref, new_tables_hbm, new_accums_hbm, new, out_sems, accums_sem):
    rows_dev = tables_ref.shape[1]
    piece = rows_dev // PIECES
    accums_out = pltpu.make_async_copy(accums_ref, new_accums_hbm, accums_sem)
    accums_out.start()

    def out(t, i):
        at = pl.ds(i * piece, piece)
        return pltpu.make_async_copy(new.at[t, at], new_tables_hbm.at[t, at], out_sems.at[t, i])

    for t in range(2):
        for i in range(PIECES):
            at = slice(i * piece, (i + 1) * piece)
            new[t, at] = tables_ref[t, at] - jnp.dot(
                onehot_ref[t, at], parts_ref[t], preferred_element_type=jnp.float32
            )
            out(t, i).start()
    accums_out.wait()
    for t in range(2):
        for i in range(PIECES):
            out(t, i).wait()


def local_step(n_group, n_local, lookup_grads, slot_index, unique_rows, tables, accums):
    look, width = lookup_grads.shape
    slots = unique_rows.shape[1]
    capacity = slots // n_group
    n_dev = n_group * n_local
    rows_dev = tables.shape[1]
    peers = n_local // BLOCKS
    vmem = pl.BlockSpec(memory_space=pltpu.VMEM)
    hbm = pl.BlockSpec(memory_space=pltpu.HBM)
    dma = pltpu.SemaphoreType.DMA
    regular = pltpu.SemaphoreType.REGULAR
    prepared = pl.pallas_call(
        functools.partial(exchange_kernel, n_group, n_local),
        out_shape=(
            pltpu.VMEM((2, 3 * slots, width), jnp.bfloat16),
            pltpu.VMEM((2, rows_dev, 3 * slots), jnp.bfloat16),
            pltpu.VMEM(tables.shape, jnp.float32),
            pltpu.VMEM(accums.shape, jnp.float32),
        ),
        in_specs=[hbm] * 5,
        out_specs=(vmem, vmem, vmem, vmem),
        scratch_shapes=[
            pltpu.VMEM((look, width), jnp.bfloat16),
            pltpu.VMEM((2, look), jnp.int32),
            pltpu.VMEM((2, slots), jnp.int32),
            pltpu.VMEM((2, rows_dev), jnp.float32),
            pltpu.VMEM((n_dev, 2, capacity, width), jnp.float32),
            pltpu.VMEM(((BLOCKS - 1) * n_group * (peers - 1), 2, capacity, width), jnp.float32),
            pltpu.VMEM((n_group, 2, capacity, width), jnp.float32),
            pltpu.VMEM((peers * (n_group - n_group // 2), 2, capacity, width), jnp.float32),
            pltpu.VMEM((n_group * (3 + peers), 2, capacity, width), jnp.float32),
            pltpu.VMEM((n_group, 2, slots), jnp.int32),
            pltpu.VMEM((4 * (n_group // 2) * capacity, width), jnp.float32),
            pltpu.VMEM((2, slots, 3 * slots), jnp.bfloat16),
            pltpu.VMEM((2, slots, rows_dev), jnp.float32),
            pltpu.VMEM((2, slots, 128), jnp.float32),
            dma((2,)), dma, dma, dma, dma,
            dma(((BLOCKS - 1) * n_group,)), dma((n_group,)), dma,
            dma, dma, dma, dma, dma, regular, regular,
        ],
        compiler_params=pltpu.CompilerParams(
            collective_id=0, has_side_effects=True, vmem_limit_bytes=48 * 2**20
        ),
        cost_estimate=pl.CostEstimate(flops=2 * 2 * look * width * slots * n_local, bytes_accessed=2 * look * width, transcendentals=0),
    )(*[pltpu.with_memory_space_constraint(x, pltpu.HBM) for x in (lookup_grads, slot_index, unique_rows, tables, accums)])
    return pl.pallas_call(
        update_kernel,
        out_shape=(
            jax.ShapeDtypeStruct(tables.shape, jnp.float32),
            jax.ShapeDtypeStruct(accums.shape, jnp.float32),
        ),
        in_specs=[vmem] * 4,
        out_specs=(hbm, hbm),
        scratch_shapes=[
            pltpu.VMEM((2, rows_dev, width), jnp.float32),
            dma((2, PIECES)), dma,
        ],
        compiler_params=pltpu.CompilerParams(vmem_limit_bytes=16 * 2**20),
    )(*prepared)


def solution(mesh):
    n_group, n_local = mesh.shape["group"], mesh.shape["local"]
    return jax.shard_map(
        functools.partial(local_step, n_group, n_local),
        mesh=mesh,
        in_specs=(
            P(("group", "local"), None),
            P(None, ("group", "local")),
            P(None, ("group", "local")),
            P(None, ("group", "local"), None),
            P(None, ("group", "local")),
        ),
        out_specs=(P(None, ("group", "local"), None), P(None, ("group", "local"))),
        check_vma=False,
    )
```
